32 devices in a mesh: dom: 16 (over z, y, core), sub: 2 (over x).
Axes of the slice: x: 2, y: 2, z: 4, core: 2. Of those that a mesh axis runs over, the one named last changes fastest.
Arguments:
- dofs: float32 [9, 56, 512], P(None, None, ('dom', 'sub')), may hold values from -6 to 6
- stiffness: float32 [3, 56, 56], replicated, may hold values from -0.75 to 0.75
- projection: float32 [4, 21, 56], replicated, may hold values from -0.75 to 0.75
- star: float32 [3, 9, 9, 512], P(None, None, None, ('dom', 'sub')), may hold values from -1.25 to 1.25
- flux_minus: float32 [4, 9, 9, 512], P(None, None, None, ('dom', 'sub')), may hold values from -1 to 1
- flux_plus: float32 [4, 9, 9, 512], P(None, None, None, ('dom', 'sub')), may hold values from -1 to 1
- fault_flux: float32 [9, 9], replicated, may hold values from -2 to 2
- fault_faces: int32 [4, 512], P(None, ('dom', 'sub')), may hold values 0 or 1
- levels: int32 [512], P(('dom', 'sub')), may hold values from 0 to 1, as said below
- face_source: int32 [4, 512], P(None, ('dom', 'sub')), may hold values from 0 to 87, as said below
- send_source: int32 [128], P(('dom', 'sub')), may hold values from 0 to 63
Outputs:
- dofs_after: float32 [9, 56, 512], P(None, None, ('dom', 'sub'))
The draws below stay inside these ranges and needn't reach their ends.
Inputs may be any that keep to these rules, and one draw needn't show every extreme that they name: `levels`: on every device at most 8 of its 16 elements have level 0, and some device has exactly 8. `face_source`: values below 64 name a face of the same device as face times 16 plus element; larger values name received exported faces as defined in the reference program.
All inputs are finite; a program needn't handle non-finite values. No bound on the sum of `fault_faces` on one device may be relied on, other than what follows from the above.
Results may differ from the reference program's by a relative error of at most 0.0001.
Values sent between devices are 32-bit elements; how exact they have to be, the bound alone decides.
A program may use at most 64 MiB of HBM per device.

```python
import math
import jax
import jax.numpy as jnp
from jax import lax

VARS = 9
MODES = 56
FACE_MODES = 21
ORDER = 6
E_DEV = 16
SEND = 4
FINE_MOST = 8
RECV = 24
ELEMS = 512
N_DOM = 16
N_SUB = 2
DEVICES = 32


def draw_levels(key, part):
    device_count = ELEMS // E_DEV
    key_count, key_busiest, key_ranks = jax.random.split(key, 3)
    counts = jax.random.randint(key_count, (device_count,), FINE_MOST // 4, FINE_MOST + 1)
    busiest = jax.random.randint(key_busiest, (), 0, device_count)
    counts = jnp.where(jnp.arange(device_count) == busiest, FINE_MOST, counts)
    ranks = jax.vmap(lambda single: jax.random.permutation(single, E_DEV))(jax.random.split(key_ranks, device_count))
    return jnp.where(ranks < counts[:, None], 0, 1).astype(jnp.int32).reshape(-1)


def draw_face_source(key, part):
    key_kind, key_local, key_remote = jax.random.split(key, 3)
    grid_shape = (4, ELEMS)
    choose_kind = jax.random.randint(key_kind, grid_shape, 0, 4)
    local_codes = jax.random.randint(key_local, grid_shape, 0, 4 * E_DEV)
    remote_codes = 4 * E_DEV + jax.random.randint(key_remote, grid_shape, 0, RECV)
    return jnp.where(choose_kind < 3, local_codes, remote_codes).astype(jnp.int32)


def touch_ends(result, key, least, high):
    extent = result.shape
    index_at = [jax.random.randint(jax.random.fold_in(key, axis), (), 0, extent[axis]) for axis in range(len(extent))]
    result = result.at[tuple(index_at)].set(least)
    longest = extent.index(max(extent))
    index_at[longest] = (index_at[longest] + 1) % extent[longest]
    return result.at[tuple(index_at)].set(high)


def block_scale(key, shape, cuts, least, largest):
    gain = 1.0
    for dim, blocks in cuts:
        heights = jax.random.uniform(jax.random.fold_in(jax.random.fold_in(key, 6), dim), (blocks,), jnp.float32, least / len(cuts), largest / len(cuts))
        gain = gain * jnp.repeat(jnp.exp(heights), shape[dim] // blocks).reshape((-1,) + (1,) * (len(shape) - 1 - dim))
    return gain


def bell_draw(stream_key, extent, width, most, cuts=(), kind=jnp.bfloat16):
    values = width * jax.random.normal(stream_key, extent, jnp.float32)
    if cuts:
        values = values * block_scale(stream_key, extent, cuts, -0.22, 0.18)
    return jnp.clip(values, -most, most).astype(kind)


def setup_inputs(seed: int = 0) -> dict:
    arg_keys = jax.random.split(jax.random.key(seed), 12)
    dofs = bell_draw(arg_keys[0], (VARS, MODES, ELEMS), 1.0, 6.0, ((2, 32),), jnp.float32)
    stiffness = bell_draw(arg_keys[1], (3, MODES, MODES), MODES ** -0.5, 0.75, (), jnp.float32)
    projection = bell_draw(arg_keys[2], (4, FACE_MODES, MODES), MODES ** -0.5, 0.75, (), jnp.float32)
    star = bell_draw(arg_keys[3], (3, VARS, VARS, ELEMS), 27 ** -0.5, 1.25, ((3, 32),), jnp.float32)
    flux_minus = bell_draw(arg_keys[4], (4, VARS, VARS, ELEMS), 36 ** -0.5, 1.0, ((3, 32),), jnp.float32)
    flux_plus = bell_draw(arg_keys[5], (4, VARS, VARS, ELEMS), 36 ** -0.5, 1.0, ((3, 32),), jnp.float32)
    fault_flux = bell_draw(arg_keys[6], (VARS, VARS), 9 ** -0.5, 2.0, (), jnp.float32)
    fault_faces = touch_ends((jax.random.randint(arg_keys[7], (4, ELEMS), 0, 8) < 1).astype(jnp.int32), jax.random.fold_in(arg_keys[7], 1), 0, 1)
    levels = draw_levels(jax.random.fold_in(arg_keys[11], 71), 0)
    face_source = draw_face_source(jax.random.fold_in(arg_keys[11], 71), 0)
    send_source = touch_ends(jax.random.randint(arg_keys[10], (SEND * DEVICES,), 0, 4 * E_DEV), jax.random.fold_in(arg_keys[10], 1), 0, (4 * E_DEV) - 1).astype(jnp.int32)
    return dict(dofs=dofs, stiffness=stiffness, projection=projection, star=star, flux_minus=flux_minus, flux_plus=flux_plus, fault_flux=fault_flux, fault_faces=fault_faces, levels=levels, face_source=face_source, send_source=send_source)


fine_step = 0.75
exact_reference = lax.Precision.HIGHEST


def taylor_weights(start_time, stop_time, term_count):
    return [(stop_time ** (term + 1) - start_time ** (term + 1)) / math.factorial(term + 1) for term in range(term_count)]


def derivatives(state_now, stiffness, star_contribution):
    taylor_series = [state_now]
    for repeat in range(ORDER - 1):
        time_slopes = jnp.einsum("dmn,wne->dwme", stiffness, taylor_series[-1], precision=exact_reference)
        taylor_series.append(jnp.einsum("usij,uifj->sfj", star_contribution, time_slopes, precision=exact_reference))
    return jnp.stack(taylor_series)


def integrate(taylor_series, start_time, stop_time):
    quadrature_weights = jnp.array(taylor_weights(start_time, stop_time, taylor_series.shape[0]), jnp.float32)
    return jnp.einsum("h,hlui->lui", quadrature_weights, taylor_series, precision=exact_reference)


def face_values(field_state, projection):
    return jnp.einsum("bly,qyp->qlbp", projection, field_state, precision=exact_reference)


def advance(state_now, own_part, own_faces, beside, stiffness, projection, star_contribution, minus_part, coupling_part):
    incoming_flux = jnp.einsum("dvwe,wne->dvne", star_contribution, own_part, precision=exact_reference)
    volume_term = jnp.einsum("utx,uytz->yxz", stiffness, incoming_flux, precision=exact_reference)
    flux_terms = jnp.einsum("fvwe,wjfe->vjfe", minus_part, own_faces, precision=exact_reference)
    flux_terms = flux_terms + jnp.einsum("fvwe,wjfe->vjfe", coupling_part, beside, precision=exact_reference)
    surface_term = jnp.einsum("alz,qlad->qzd", projection, flux_terms, precision=exact_reference)
    return state_now + volume_term - surface_term


def to_blocks(array):
    split = array.reshape(array.shape[:-1] + (ELEMS // E_DEV, E_DEV))
    return jnp.moveaxis(split, -2, 0)


def from_blocks(array):
    joined = jnp.moveaxis(array, 0, -2)
    return joined.reshape(joined.shape[:-2] + (ELEMS,))


def reference(dofs, stiffness, projection, star, flux_minus, flux_plus, fault_flux, fault_faces, levels, face_source, send_source):
    device_count = ELEMS // E_DEV
    coupling = jnp.where(fault_faces[:, None, None, :] == 1, fault_flux[None, :, :, None], flux_plus)
    element_ids = jnp.arange(ELEMS, dtype=jnp.int32)
    device_ids = (element_ids // E_DEV)[None, :]
    local_column = device_ids * (4 * E_DEV) + face_source
    offset = face_source - 4 * E_DEV
    side_index = offset // (N_SUB * SEND)
    sub_index = (offset // SEND) % N_SUB
    slot_index = offset % SEND
    source_device = ((device_ids // N_SUB + side_index - 1) % N_DOM) * N_SUB + sub_index
    send_position = jnp.clip(source_device * SEND + slot_index, 0, device_count * SEND - 1).astype(jnp.int32)
    remote_column = source_device * (4 * E_DEV) + send_source[send_position]
    column = jnp.where(face_source < 4 * E_DEV, local_column, remote_column).astype(jnp.int32)
    column_order = to_blocks(column).reshape(-1)

    def beside_values(face_blocks):
        source_table = jnp.moveaxis(face_blocks, 0, 2).reshape(VARS * FACE_MODES, -1)
        picked = jnp.take(source_table, column_order, axis=1)
        return jnp.moveaxis(picked.reshape(VARS, FACE_MODES, device_count, 4, E_DEV), 2, 0)

    block_dofs = to_blocks(dofs)
    block_star = to_blocks(star)
    block_minus = to_blocks(flux_minus)
    block_coupling = to_blocks(coupling)
    block_fine = to_blocks(levels == 0)

    def phase_one(items):
        state_now, star_contribution = items
        taylor_series = derivatives(state_now, stiffness, star_contribution)
        first_half = integrate(taylor_series, 0.0, fine_step)
        second_half = integrate(taylor_series, fine_step, 2.0 * fine_step)
        return first_half, second_half, face_values(first_half, projection)

    first_b, second_b, first_faces_b = lax.map(phase_one, (block_dofs, block_star))
    beside_first_b = beside_values(first_faces_b)

    def phase_two(items):
        state_now, star_contribution, minus_part, coupling_part, is_fine, first_half, second_half, first_faces, beside_first = items
        updated = advance(state_now, first_half, first_faces, beside_first, stiffness, projection, star_contribution, minus_part, coupling_part)
        state_one = jnp.where(is_fine, updated, state_now)
        fine_integral = integrate(derivatives(state_one, stiffness, star_contribution), 0.0, fine_step)
        carried = jnp.where(is_fine, fine_integral, second_half)
        return state_one, carried, face_values(carried, projection)

    state_one_b, carried_b, carried_faces_b = lax.map(phase_two, (block_dofs, block_star, block_minus, block_coupling, block_fine, first_b, second_b, first_faces_b, beside_first_b))
    beside_carried_b = beside_values(carried_faces_b)

    def phase_three(items):
        state_now, star_contribution, minus_part, coupling_part, is_fine, first_half, second_half, beside_first, state_one, carried, carried_faces, beside_carried = items
        fine_new = advance(state_one, carried, carried_faces, beside_carried, stiffness, projection, star_contribution, minus_part, coupling_part)
        whole_step = first_half + second_half
        coarse_new = advance(state_now, whole_step, face_values(whole_step, projection), beside_first + beside_carried, stiffness, projection, star_contribution, minus_part, coupling_part)
        return jnp.where(is_fine, fine_new, coarse_new)

    result_b = lax.map(phase_three, (block_dofs, block_star, block_minus, block_coupling, block_fine, first_b, second_b, beside_first_b, state_one_b, carried_b, carried_faces_b, beside_carried_b))
    return from_blocks(result_b)
```

```python
import functools
import math

import jax
import jax.numpy as jnp
from jax import lax
from jax.experimental import pallas as pl
from jax.experimental.pallas import tpu as pltpu
from jax.sharding import PartitionSpec as P

MESH = pl.DeviceIdType.MESH
ORDER = 6
fine_step = 0.75
F32 = jnp.float32
BF16 = jnp.bfloat16
SUB = 8
LANES = 128


def taylor_weights(start_time, stop_time, term_count):
    return [
        (stop_time ** (term + 1) - start_time ** (term + 1)) / math.factorial(term + 1)
        for term in range(term_count)
    ]


def up_to(value, step):
    return -(-value // step) * step


def dot(a, b):
    return jnp.dot(a, b, preferred_element_type=F32)


def take(value, index):
    return jnp.take_along_axis(value, index, axis=1, mode="promise_in_bounds")


def total_of(parts):
    return functools.reduce(lambda a, b: a + b, parts)


def both(tiles):
    parts = []
    for tile in tiles:
        high = tile.astype(BF16).astype(F32)
        parts += [high, tile - high]
    return jnp.concatenate(parts, axis=0).astype(BF16)


def product(columns, weights):
    lhs = jnp.concatenate([both(tiles) for tiles in columns], axis=1)
    out = dot(lhs, weights)
    half = weights.shape[1] // 2
    result = []
    for v in range(len(columns[0])):
        at = 2 * SUB * v
        result.append(
            out[at : at + SUB, :half]
            + out[at : at + SUB, half:]
            + out[at + SUB : at + 2 * SUB, :half]
        )
    return result


def kernel(
    sizes,
    dofs_hbm,
    stiffness_hbm,
    projection_hbm,
    star_hbm,
    minus_hbm,
    plus_hbm,
    fault_hbm,
    fault_faces_hbm,
    levels_hbm,
    face_source_hbm,
    send_source_hbm,
    out,
    dofs,
    stiffness,
    projection,
    star,
    flux_minus,
    flux_plus,
    fault_flux,
    fault_faces,
    levels,
    face_source,
    send_source,
    rows,
    packed,
    ints,
    square,
    fault_rows,
    diagonal,
    spread_projection,
    star_coef,
    minus_coef,
    plus_coef,
    series_weights,
    back_weights,
    face_weights,
    faces_ref,
    export,
    received,
    load_sem,
    send_sem,
    recv_sem,
):
    n_dom, n_sub = sizes
    var_count, elems, modes = dofs.shape
    dims = stiffness.shape[0]
    face_modes, faces = projection.shape[0], projection.shape[1]
    slots = send_source.shape[1]
    halves = elems // SUB
    m_block = LANES // halves
    j_block = LANES // max(faces, slots)
    sources = 3 * n_sub
    pairs = var_count * var_count
    pitch = rows.shape[0] // packed.shape[0]

    loads = [
        pltpu.make_async_copy(src, dst, load_sem.at[i])
        for i, (src, dst) in enumerate(
            (
                (star_hbm, star),
                (stiffness_hbm, stiffness),
                (dofs_hbm, dofs),
                (projection_hbm, projection),
                (face_source_hbm, face_source),
                (send_source_hbm, send_source),
                (levels_hbm, levels),
                (fault_faces_hbm, fault_faces),
                (fault_hbm, fault_flux),
                (minus_hbm, flux_minus),
                (plus_hbm, flux_plus),
            )
        )
    ]
    for load in loads:
        load.start()

    me_dom, me_sub = lax.axis_index("dom"), lax.axis_index("sub")
    partners = []
    for delta in (-1, 0, 1):
        for turn in range(n_sub):
            if delta or turn:
                partners.append(
                    (
                        (
                            lax.rem(me_dom + delta + n_dom, n_dom),
                            lax.rem(me_sub + turn, n_sub),
                        ),
                        (1 - delta) * n_sub + me_sub,
                    )
                )
    barrier = pltpu.get_barrier_semaphore()
    for target, _ in partners:
        pl.semaphore_signal(barrier, inc=1, device_id=target, device_id_type=MESH)

    diagonal[...] = jnp.zeros_like(diagonal)
    spread_projection[...] = jnp.zeros_like(spread_projection)
    ints[...] = jnp.zeros_like(ints)
    square[...] = jnp.zeros_like(square)

    sublane = lax.broadcasted_iota(jnp.int32, (SUB, LANES), 0)
    lane = lax.broadcasted_iota(jnp.int32, (SUB, LANES), 1)
    mode_half = lane // m_block
    face_lane = lane // j_block
    inside = lane % j_block
    star_index = mode_half * SUB + sublane
    flux_index = [face_lane * j_block + h * SUB + sublane for h in range(halves)]

    def row_of(ref, at):
        return jnp.broadcast_to(ref[at : at + 1, :], (SUB, LANES))

    loads[0].wait()
    for v in range(var_count):
        for w in range(var_count):
            at = (v * var_count + w) * pitch
            rows[at : at + dims, 0:elems] = star[v, w]
    for d in range(dims):
        for pair in range(pairs):
            star_coef[d, pair] = take(row_of(rows, pair * pitch + d), star_index)

    loads[1].wait()
    for d in range(dims):
        for h in range(halves):
            at = slice(h * m_block, h * m_block + modes)
            diagonal[d, at, at] = stiffness[d]

    def put(ref, at, value):
        high = value.astype(BF16)
        count, width = value.shape
        ref[at : at + count, 0:width] = high
        ref[at : at + count, width : 2 * width] = (value - high.astype(F32)).astype(BF16)

    for d in range(dims):
        put(series_weights, d * LANES, jnp.transpose(diagonal[d]))

    loads[2].wait()
    state = []
    for v in range(var_count):
        parts = []
        for h in range(halves):
            parts.append(dofs[v, h * SUB : (h + 1) * SUB, :])
            if m_block > modes:
                parts.append(jnp.zeros((SUB, m_block - modes), F32))
        state.append(jnp.concatenate(parts, axis=1))

    def mixed(tiles):
        return [
            [
                total_of(
                    [
                        star_coef[d, v * var_count + w] * tiles[w]
                        for w in range(var_count)
                    ]
                )
                for v in range(var_count)
            ]
            for d in range(dims)
        ]

    def series(value, weight_sets):
        totals = [[weights[0] * tile for tile in value] for weights in weight_sets]
        for term in range(1, ORDER):
            value = product(mixed(value), series_weights[...])
            totals = [
                [total + weights[term] * tile for total, tile in zip(sums, value)]
                for sums, weights in zip(totals, weight_sets)
            ]
        return totals

    first_weights = taylor_weights(0.0, fine_step, ORDER)
    second_weights = taylor_weights(fine_step, 2.0 * fine_step, ORDER)

    for i in range(3, 8):
        loads[i].wait()
    for h in range(halves):
        for f in range(faces):
            at = h * LANES + f * j_block
            spread_projection[
                at : at + face_modes, h * m_block : h * m_block + modes
            ] = projection[:, f, :]
    put(face_weights, 0, jnp.transpose(spread_projection[...]))
    for f in range(faces):
        at = slice(f * j_block, f * j_block + elems)
        ints[0:1, at] = face_source[f : f + 1, :]
        ints[1:2, at] = fault_faces[f : f + 1, :]
    ints[2:3, 0:elems] = levels[...]
    ints[3:4, 0:slots] = send_source[...]
    codes = [take(row_of(ints, 0), flux_index[h]) for h in range(halves)]
    fine = take(row_of(ints, 2), star_index) == 0
    sent = take(row_of(ints, 3), face_lane)
    sent_index = (sent // elems) * j_block + inside
    sent_elem = sent % elems

    first_half, second_half = series(state, (first_weights, second_weights))

    def face_values(tiles):
        wide = product([tiles], face_weights[...])
        return [
            [tile[:, h * LANES : (h + 1) * LANES] for h in range(halves)] for tile in wide
        ]

    own_slot = n_sub + me_sub

    def launch(phase, values):
        for v in range(var_count):
            picked = total_of(
                [
                    jnp.where(
                        sent_elem == h * SUB + sublane, take(values[v][h], sent_index), 0.0
                    )
                    for h in range(halves)
                ]
            )
            export[phase, v : v + 1, :] = jnp.sum(picked, axis=0, keepdims=True)
        copies = []
        for i, (target, slot) in enumerate(partners):
            copy = pltpu.make_async_remote_copy(
                src_ref=export.at[phase],
                dst_ref=received.at[phase, slot],
                send_sem=send_sem.at[phase, i],
                recv_sem=recv_sem.at[phase, i],
                device_id=target,
                device_id_type=MESH,
            )
            copy.start()
            copies.append(copy)
        received[phase, own_slot] = export[phase]
        return copies

    local_index, local_elem, far_index, far_source = [], [], [], []
    for h in range(halves):
        local = codes[h] < faces * elems
        far = codes[h] - faces * elems
        local_index.append(jnp.where(local, codes[h] // elems, 0) * j_block + inside)
        local_elem.append(jnp.where(local, codes[h] % elems, -1))
        far_index.append(jnp.where(local, 0, far % slots) * j_block + inside)
        far_source.append(jnp.where(local, -1, far // slots))

    def flux_of(coef, values, h):
        return [
            total_of(
                [
                    coef[h, v * var_count + w] * values[w][h]
                    for w in range(var_count)
                ]
            )
            for v in range(var_count)
        ]

    def local_part(value, values):
        for v in range(var_count):
            for h in range(halves):
                faces_ref[v, h] = values[v][h]
        beside = [[jnp.zeros((SUB, LANES), F32)] * halves for _ in range(var_count)]
        for v in range(var_count):
            for e in range(elems):
                row = jnp.broadcast_to(
                    faces_ref[v, e // SUB, e % SUB : e % SUB + 1, :], (SUB, LANES)
                )
                for h in range(halves):
                    beside[v][h] = jnp.where(
                        local_elem[h] == e, take(row, local_index[h]), beside[v][h]
                    )
        own = [flux_of(minus_coef, values, h) for h in range(halves)]
        return beside, product(mixed(value) + own, back_weights[...])

    def finish(phase, copies, start, beside, parts):
        for copy in copies:
            copy.wait_recv()
        for v in range(var_count):
            for k in range(sources):
                row = jnp.broadcast_to(received[phase, k, v : v + 1, :], (SUB, LANES))
                for h in range(halves):
                    beside[v][h] = jnp.where(
                        far_source[h] == k, take(row, far_index[h]), beside[v][h]
                    )
        flux = [flux_of(plus_coef, beside, h) for h in range(halves)]
        last = product(flux, back_weights[dims * LANES :, :])
        return [a + b + c for a, b, c in zip(start, parts, last)]

    values = face_values(first_half)
    pl.semaphore_wait(barrier, len(partners))
    copies = launch(0, values)

    for i in range(8, 11):
        loads[i].wait()
    for d in range(dims):
        put(back_weights, d * LANES, diagonal[d])
    put(back_weights, dims * LANES, -spread_projection[...])

    def pack(source):
        for v in range(var_count):
            for w in range(var_count):
                at = (v * var_count + w) * pitch
                rows[at : at + faces, 0:elems] = source[v, w]
        count = packed.shape[0]
        block = lax.broadcasted_iota(jnp.int32, (count, LANES), 1) // j_block
        value = rows[pl.ds(0, count, stride=pitch), :]
        for f in range(1, faces):
            part = rows[pl.ds(f, count, stride=pitch), :]
            value = jnp.where(block == f, pltpu.roll(part, f * j_block, 1), value)
        return value

    packed[...] = pack(flux_minus)
    for pair in range(pairs):
        row = row_of(packed, pair)
        for h in range(halves):
            minus_coef[h, pair] = take(row, flux_index[h])

    square[0:var_count, 0:var_count] = fault_flux[...]
    turned = jnp.transpose(square[...])[0 : up_to(var_count, SUB)]
    for v in range(var_count):
        column = jnp.broadcast_to(turned[:, v : v + 1], (turned.shape[0], LANES))
        fault_rows[v * var_count : (v + 1) * var_count, :] = column[0:var_count]
    on_fault = jnp.broadcast_to(ints[1:2, :], packed.shape) == 1
    packed[...] = jnp.where(on_fault, fault_rows[...], pack(flux_plus))
    for pair in range(pairs):
        row = row_of(packed, pair)
        for h in range(halves):
            plus_coef[h, pair] = take(row, flux_index[h])

    beside, parts = local_part(first_half, values)
    moved = finish(0, copies, state, beside, parts)
    (fine_half,) = series(moved, (first_weights,))
    carried = [jnp.where(fine, a, b) for a, b in zip(fine_half, second_half)]
    values = face_values(carried)
    last_copies = launch(1, values)
    beside, parts = local_part(carried, values)
    result = finish(1, last_copies, moved, beside, parts)
    for v in range(var_count):
        for h in range(halves):
            out[v, h * SUB : (h + 1) * SUB, :] = result[v][
                :, h * m_block : h * m_block + modes
            ]
    for copy in copies + last_copies:
        copy.wait_send()


def solution(mesh):
    n_dom, n_sub = mesh.shape["dom"], mesh.shape["sub"]

    def per_device(
        dofs,
        stiffness,
        projection,
        star,
        flux_minus,
        flux_plus,
        fault_flux,
        fault_faces,
        levels,
        face_source,
        send_source,
    ):
        var_count, modes, elems = dofs.shape
        dims = stiffness.shape[0]
        faces, face_modes = projection.shape[0], projection.shape[1]
        halves = elems // SUB
        pairs = var_count * var_count
        count = up_to(pairs, SUB)
        pitch = max(dims, faces)
        sources = 3 * n_sub
        moved = [
            jnp.transpose(dofs, (0, 2, 1)),
            stiffness,
            jnp.transpose(projection, (1, 0, 2)),
            jnp.transpose(star, (1, 2, 0, 3)),
            jnp.transpose(flux_minus, (1, 2, 0, 3)),
            jnp.transpose(flux_plus, (1, 2, 0, 3)),
            fault_flux,
            fault_faces,
            levels.reshape(1, -1),
            face_source,
            send_source.reshape(1, -1),
        ]
        result = pl.pallas_call(
            functools.partial(kernel, (n_dom, n_sub)),
            out_shape=pltpu.VMEM((var_count, elems, modes), F32),
            in_specs=[pl.BlockSpec(memory_space=pltpu.HBM)] * len(moved),
            out_specs=pl.BlockSpec(memory_space=pltpu.VMEM),
            scratch_shapes=[pltpu.VMEM(one.shape, one.dtype) for one in moved]
            + [
                pltpu.VMEM((count * pitch, LANES), F32),
                pltpu.VMEM((count, LANES), F32),
                pltpu.VMEM((SUB, LANES), jnp.int32),
                pltpu.VMEM((LANES, LANES), F32),
                pltpu.VMEM((count, LANES), F32),
                pltpu.VMEM((dims, LANES, LANES), F32),
                pltpu.VMEM((halves * LANES, LANES), F32),
                pltpu.VMEM((dims, pairs, SUB, LANES), F32),
                pltpu.VMEM((halves, pairs, SUB, LANES), F32),
                pltpu.VMEM((halves, pairs, SUB, LANES), F32),
                pltpu.VMEM((dims * LANES, 2 * LANES), BF16),
                pltpu.VMEM(((dims + halves) * LANES, 2 * LANES), BF16),
                pltpu.VMEM((LANES, 2 * halves * LANES), BF16),
                pltpu.VMEM((var_count, halves, SUB, LANES), F32),
                pltpu.VMEM((2, var_count, LANES), F32),
                pltpu.VMEM((2, sources, var_count, LANES), F32),
                pltpu.SemaphoreType.DMA((len(moved),)),
                pltpu.SemaphoreType.DMA((2, sources - 1)),
                pltpu.SemaphoreType.DMA((2, sources - 1)),
            ],
            compiler_params=pltpu.CompilerParams(
                collective_id=0,
                has_side_effects=True,
                vmem_limit_bytes=66_000_000,
            ),
            name="window",
        )(*moved)
        return jnp.transpose(result, (0, 2, 1))

    return jax.shard_map(
        per_device,
        mesh=mesh,
        in_specs=(
            P(None, None, ("dom", "sub")),
            P(),
            P(),
            P(None, None, None, ("dom", "sub")),
            P(None, None, None, ("dom", "sub")),
            P(None, None, None, ("dom", "sub")),
            P(),
            P(None, ("dom", "sub")),
            P(("dom", "sub")),
            P(None, ("dom", "sub")),
            P(("dom", "sub")),
        ),
        out_specs=P(None, None, ("dom", "sub")),
        check_vma=False,
    )
```

```python
import functools
import math

import jax
import jax.numpy as jnp
from jax import lax
from jax.experimental import pallas as pl
from jax.experimental.pallas import tpu as pltpu
from jax.sharding import PartitionSpec as P

MESH = pl.DeviceIdType.MESH
ORDER = 6
fine_step = 0.75
F32 = jnp.float32
BF16 = jnp.bfloat16
SUB = 8
LANES = 128


def taylor_weights(start_time, stop_time, term_count):
    return [
        (stop_time ** (term + 1) - start_time ** (term + 1)) / math.factorial(term + 1)
        for term in range(term_count)
    ]


def up_to(value, step):
    return -(-value // step) * step


def dot(a, b):
    return jnp.dot(a, b, preferred_element_type=F32)


def take(value, index):
    return jnp.take_along_axis(value, index, axis=1, mode="promise_in_bounds")


def total_of(parts):
    return functools.reduce(lambda a, b: a + b, parts)


def both(tiles):
    parts = []
    for tile in tiles:
        high = tile.astype(BF16).astype(F32)
        parts += [high, tile - high]
    return jnp.concatenate(parts, axis=0).astype(BF16)


def product(columns, weights):
    lhs = jnp.concatenate([both(tiles) for tiles in columns], axis=1)
    out = dot(lhs, weights)
    half = weights.shape[1] // 2
    result = []
    for v in range(len(columns[0])):
        at = 2 * SUB * v
        result.append(
            out[at : at + SUB, :half]
            + out[at : at + SUB, half:]
            + out[at + SUB : at + 2 * SUB, :half]
        )
    return result


def kernel(
    sizes,
    dofs_hbm,
    stiffness_hbm,
    projection_hbm,
    star_hbm,
    minus_hbm,
    plus_hbm,
    fault_hbm,
    fault_faces_hbm,
    levels_hbm,
    face_source_hbm,
    send_source_hbm,
    out,
    dofs,
    stiffness,
    projection,
    star,
    flux_minus,
    flux_plus,
    fault_flux,
    fault_faces,
    levels,
    face_source,
    send_source,
    star_lines,
    minus_lines,
    plus_lines,
    packed_star,
    packed_minus,
    packed_plus,
    ints,
    square,
    fault_rows,
    diagonal,
    spread_projection,
    star_coef,
    minus_coef,
    plus_coef,
    series_weights,
    back_weights,
    face_weights,
    faces_ref,
    part_ref,
    guest_star,
    guest_plus,
    guest_star_coef,
    guest_plus_coef,
    guest_rows,
    early_out,
    early_in,
    near_out,
    near_in,
    first_out,
    first_in,
    load_sem,
    early_send,
    early_recv,
    near_send,
    near_recv,
    first_send,
    first_recv,
):
    n_dom, n_sub = sizes
    var_count, elems, modes = dofs.shape
    dims = stiffness.shape[0]
    face_modes, faces = projection.shape[0], projection.shape[1]
    slots = send_source.shape[1]
    halves = elems // SUB
    m_block = LANES // halves
    j_block = LANES // max(faces, slots)
    quarters = LANES // j_block
    pairs = var_count * var_count
    pitch = star_lines.shape[0] // packed_star.shape[0]
    deep = packed_star.shape[0] // quarters
    stack = SUB // slots
    per_set = stack * halves
    per_group = j_block // slots

    near = [
        (delta, turn)
        for delta in (-1, 1, 0)
        for turn in range(n_sub)
        if delta or turn
    ]
    wide = [
        (delta, turn)
        for delta in (-2, -1, 0, 1, 2)
        for turn in range(n_sub)
        if delta or turn
    ]
    tiles = -(-len(near) // stack)
    sets = -(-tiles // halves)

    def place(delta, turn):
        return (delta + 2) * n_sub + turn % n_sub

    loads = [
        pltpu.make_async_copy(src, dst, load_sem.at[i])
        for i, (src, dst) in enumerate(
            (
                (star_hbm, star),
                (stiffness_hbm, stiffness),
                (dofs_hbm, dofs),
                (projection_hbm, projection),
                (face_source_hbm, face_source),
                (send_source_hbm, send_source),
                (levels_hbm, levels),
                (fault_faces_hbm, fault_faces),
                (fault_hbm, fault_flux),
                (plus_hbm, flux_plus),
                (minus_hbm, flux_minus),
            )
        )
    ]
    for load in loads:
        load.start()

    me_dom, me_sub = lax.axis_index("dom"), lax.axis_index("sub")

    def device(delta, turn):
        return (
            lax.rem(me_dom + delta + n_dom, n_dom),
            lax.rem(me_sub + turn, n_sub),
        )

    barrier = pltpu.get_barrier_semaphore()
    for delta, turn in wide:
        pl.semaphore_signal(
            barrier, inc=1, device_id=device(delta, turn), device_id_type=MESH
        )

    diagonal[...] = jnp.zeros_like(diagonal)
    spread_projection[...] = jnp.zeros_like(spread_projection)
    ints[...] = jnp.zeros_like(ints)
    square[...] = jnp.zeros_like(square)

    sublane = lax.broadcasted_iota(jnp.int32, (SUB, LANES), 0)
    lane = lax.broadcasted_iota(jnp.int32, (SUB, LANES), 1)
    mode_half = lane // m_block
    block = lane // j_block
    inside = lane % j_block
    lane_slot = lane % slots
    sub_slot = sublane % slots
    sub_stack = sublane // slots
    star_index = mode_half * SUB + sublane
    flux_index = [block * j_block + h * SUB + sublane for h in range(halves)]

    def row_of(ref, at):
        return jnp.broadcast_to(ref[at : at + 1, :], (SUB, LANES))

    loads[0].wait()

    def lines(ref, source, count):
        for v in range(var_count):
            for w in range(var_count):
                at = (v * var_count + w) * pitch
                ref[at : at + count, 0:elems] = source[v, w]

    def pack(ref, count):
        depth = packed_star.shape[0]
        where = lax.broadcasted_iota(jnp.int32, (depth, LANES), 1) // j_block
        value = ref[pl.ds(0, depth, stride=pitch), :]
        for f in range(1, count):
            part = ref[pl.ds(f, depth, stride=pitch), :]
            value = jnp.where(where == f, pltpu.roll(part, f * j_block, 1), value)
        return value

    for load in loads[1:9]:
        load.wait()
    lines(star_lines, star, dims)
    for d in range(dims):
        for pair in range(pairs):
            star_coef[d, pair] = take(row_of(star_lines, pair * pitch + d), star_index)

    for d in range(dims):
        for h in range(halves):
            at = slice(h * m_block, h * m_block + modes)
            diagonal[d, at, at] = stiffness[d]

    def put(ref, at, value):
        high = value.astype(BF16)
        count, width = value.shape
        ref[at : at + count, 0:width] = high
        ref[at : at + count, width : 2 * width] = (value - high.astype(F32)).astype(BF16)

    for d in range(dims):
        put(series_weights, d * LANES, jnp.transpose(diagonal[d]))

    state = []
    for v in range(var_count):
        parts = []
        for h in range(halves):
            parts.append(dofs[v, h * SUB : (h + 1) * SUB, :])
            if m_block > modes:
                parts.append(jnp.zeros((SUB, m_block - modes), F32))
        state.append(jnp.concatenate(parts, axis=1))

    def mixed(coef, value):
        return [
            [
                total_of(
                    [coef[d, v * var_count + w] * value[w] for w in range(var_count)]
                )
                for v in range(var_count)
            ]
            for d in range(dims)
        ]

    def step(coef, value):
        return product(mixed(coef, value), series_weights[...])

    first_weights = taylor_weights(0.0, fine_step, ORDER)
    second_weights = taylor_weights(fine_step, 2.0 * fine_step, ORDER)

    for h in range(halves):
        for f in range(faces):
            at = h * LANES + f * j_block
            spread_projection[
                at : at + face_modes, h * m_block : h * m_block + modes
            ] = projection[:, f, :]
    put(face_weights, 0, jnp.transpose(spread_projection[...]))
    for d in range(dims):
        put(back_weights, d * LANES, diagonal[d])
    put(back_weights, dims * LANES, -spread_projection[...])

    for f in range(faces):
        at = slice(f * j_block, f * j_block + elems)
        ints[0:1, at] = face_source[f : f + 1, :]
        ints[1:2, at] = fault_faces[f : f + 1, :]
    ints[2:3, 0:elems] = levels[...]
    ints[3:4, 0:slots] = send_source[...]

    raw = row_of(ints, 0)
    beyond = jnp.maximum(raw - faces * elems, 0)
    code_delta = beyond // (n_sub * slots) - 1
    code_turn = lax.rem((beyond // slots) % n_sub - me_sub + n_sub, n_sub)
    code_slot = beyond % slots
    own_export = take(row_of(ints, 3), code_slot)
    is_far = raw >= faces * elems
    is_own = is_far & (code_delta == 0) & (code_turn == 0)
    local_code = jnp.where(is_own, own_export, jnp.where(is_far, -1, raw))
    far_code = jnp.where(
        is_far & jnp.logical_not(is_own),
        ((code_delta + 1) * n_sub + code_turn) * slots + code_slot,
        -1,
    )
    local_index, local_elem, far_index, far_place = [], [], [], []
    for h in range(halves):
        local = take(local_code, flux_index[h])
        far = take(far_code, flux_index[h])
        near_by = jnp.maximum(local, 0)
        there = jnp.maximum(far, 0)
        local_index.append((near_by // elems) * j_block + inside)
        local_elem.append(jnp.where(local < 0, -1, near_by % elems))
        far_index.append((there % slots) * j_block + inside)
        far_place.append(jnp.where(far < 0, -1, there // slots + n_sub))
    fine = take(row_of(ints, 2), star_index) == 0
    sent = take(row_of(ints, 3), block)
    sent_index = (sent // elems) * j_block + inside
    sent_elem = sent % elems
    small = take(row_of(ints, 3), lane_slot)
    small_elem = small % elems
    rising = take(row_of(ints, 3), sub_slot) % elems

    square[0:var_count, 0:var_count] = fault_flux[...]
    turned = jnp.transpose(square[...])[0 : up_to(var_count, SUB)]
    for v in range(var_count):
        column = jnp.broadcast_to(turned[:, v : v + 1], (turned.shape[0], LANES))
        fault_rows[v * var_count : (v + 1) * var_count, :] = column[0:var_count]
    loads[9].wait()
    lines(plus_lines, flux_plus, faces)
    on_fault = jnp.broadcast_to(ints[1:2, :], packed_plus.shape) == 1
    packed_plus[...] = jnp.where(on_fault, fault_rows[...], pack(plus_lines, faces))
    packed_star[...] = pack(star_lines, dims)

    part_of = inside // slots
    early_star = jnp.minimum(part_of, dims - 1) * j_block + small_elem
    early_plus = jnp.clip(part_of - dims, 0, faces - 1) * j_block + small_elem
    for i in range(deep // SUB):
        value = jnp.zeros((SUB, LANES), F32)
        for q in range(quarters):
            at = slice(q * deep + i * SUB, q * deep + (i + 1) * SUB)
            one = jnp.where(
                part_of < dims,
                take(packed_star[at, :], early_star),
                take(packed_plus[at, :], early_plus),
            )
            value = jnp.where(block == q, one, value)
        early_out[i * SUB : (i + 1) * SUB, :] = value
    marks = [
        take(far_code, block * j_block + small_elem),
        jnp.where(take(row_of(ints, 2), sent_elem) == 0, 1, 0),
        small // elems,
    ]
    for i, mark in enumerate(marks):
        early_out[deep + i : deep + i + 1, :] = mark[0:1].astype(F32)

    def send(source, target, partners, index_of, send_sem, recv_sem):
        copies = []
        for i, (delta, turn) in enumerate(partners):
            copy = pltpu.make_async_remote_copy(
                src_ref=source,
                dst_ref=target.at[index_of(-delta, -turn % n_sub)],
                send_sem=send_sem.at[i],
                recv_sem=recv_sem.at[i],
                device_id=device(delta, turn),
                device_id_type=MESH,
            )
            copy.start()
            copies.append(copy)
        return copies

    def near_place(delta, turn):
        return near.index((delta, turn))

    early_at = 2
    value, firsts = state, [first_weights[0] * tile for tile in state]
    seconds = [second_weights[0] * tile for tile in state]
    early_copies = None
    for term in range(1, ORDER):
        if term == early_at:
            pl.semaphore_wait(barrier, len(wide))
            early_copies = send(
                early_out, early_in, near, near_place, early_send, early_recv
            )
            loads[10].wait()
            lines(minus_lines, flux_minus, faces)
            packed_minus[...] = pack(minus_lines, faces)
            for pair in range(pairs):
                row = row_of(packed_minus, pair)
                for h in range(halves):
                    minus_coef[h, pair] = take(row, flux_index[h])
            for pair in range(pairs):
                row = row_of(packed_plus, pair)
                for h in range(halves):
                    plus_coef[h, pair] = take(row, flux_index[h])
        value = step(star_coef, value)
        firsts = [a + first_weights[term] * b for a, b in zip(firsts, value)]
        seconds = [a + second_weights[term] * b for a, b in zip(seconds, value)]
    first_half, second_half = firsts, seconds

    def face_values(value):
        broad = product([value], face_weights[...])
        return [
            [tile[:, h * LANES : (h + 1) * LANES] for h in range(halves)]
            for tile in broad
        ]

    def export(ref, at, values):
        for v in range(var_count):
            picked = total_of(
                [
                    jnp.where(
                        sent_elem == h * SUB + sublane, take(values[v][h], sent_index), 0.0
                    )
                    for h in range(halves)
                ]
            )
            ref[at + v : at + v + 1, :] = jnp.sum(picked, axis=0, keepdims=True)

    def flux_of(coef, values):
        return [
            total_of([coef[v * var_count + w] * values[w] for w in range(var_count)])
            for v in range(var_count)
        ]

    def gather_local(values):
        for v in range(var_count):
            for h in range(halves):
                faces_ref[v, h] = values[v][h]
        beside = [[jnp.zeros((SUB, LANES), F32)] * var_count for _ in range(halves)]
        for h in range(halves):
            for v in range(var_count):
                for e in range(elems):
                    row = row_of(faces_ref.at[v, e // SUB], e % SUB)
                    beside[h][v] = jnp.where(
                        local_elem[h] == e, take(row, local_index[h]), beside[h][v]
                    )
        return beside

    values = face_values(first_half)
    export(first_out, 0, values)
    first_copies = send(first_out, first_in, wide, place, first_send, first_recv)
    own_place = place(0, 0)
    first_in[own_place] = first_out[...]

    beside = gather_local(values)
    flux = []
    for h in range(halves):
        own = flux_of(minus_coef.at[h], [values[w][h] for w in range(var_count)])
        other = flux_of(plus_coef.at[h], beside[h])
        flux.append([a + b for a, b in zip(own, other)])
    partial = [
        a + b
        for a, b in zip(
            state, product(mixed(star_coef, first_half) + flux, back_weights[...])
        )
    ]

    for v in range(var_count):
        part_ref[v] = partial[v]
    rising_half, rising_sub = rising // SUB, rising % SUB
    copied = []
    for v in range(var_count):
        row = jnp.zeros((SUB, LANES), F32)
        for e in range(SUB):
            row = jnp.where(rising_sub == e, row_of(part_ref.at[v], e), row)
        for h in range(1, halves):
            turned_row = pltpu.roll(row, h * m_block, 1)
            copied.append((row, turned_row)) if halves == 2 else None
    nears = -(-var_count // per_set)
    for t in range(nears):
        value = jnp.zeros((SUB, LANES), F32)
        for part in range(per_set):
            v = t * per_set + part
            if v < var_count:
                row, turned_row = copied[v]
                one = jnp.where(rising_half == mode_half, row, turned_row)
                here = (sub_stack == part % stack) & (mode_half == part // stack)
                value = jnp.where(here, one, value)
        near_out[t * SUB : (t + 1) * SUB, :] = value
    export(near_out, nears * SUB, face_values(second_half))
    near_copies = send(near_out, near_in, near, near_place, near_send, near_recv)

    for copy in early_copies:
        copy.wait_recv()
    groups = -(-len(near) // per_group)
    for group in range(groups):
        members = range(group * per_group, min(len(near), (group + 1) * per_group))
        for q in range(quarters):
            star_from = q * j_block + jnp.minimum(block, dims - 1) * slots + lane_slot
            plus_from = q * j_block + (dims + jnp.minimum(block, faces - 1)) * slots + lane_slot
            for i in range(deep // SUB):
                one = jnp.zeros((SUB, LANES), F32)
                two = one
                for k in members:
                    got = early_in[k, i * SUB : (i + 1) * SUB, :]
                    here = part_of == k % per_group
                    one = jnp.where(here, take(got, star_from), one)
                    two = jnp.where(here, take(got, plus_from), two)
                at = slice(q * deep + i * SUB, q * deep + (i + 1) * SUB)
                guest_star[group, at, :] = one
                guest_plus[group, at, :] = two
    from_lane = lax.broadcasted_iota(jnp.int32, (LANES, LANES), 0)
    to_half = lax.broadcasted_iota(jnp.int32, (LANES, LANES), 1) // m_block
    for group in range(groups):
        members = [s for s in range(sets) if s * per_set // per_group == group]
        picks = jnp.concatenate(
            [
                jnp.where(
                    (from_lane // j_block == d)
                    & (
                        from_lane % j_block // SUB
                        == s * per_set % per_group // stack + to_half
                    ),
                    1.0,
                    0.0,
                )
                for s in members
                for d in range(dims)
            ],
            axis=1,
        ).astype(BF16)
        for v in range(var_count):
            chosen = []
            for w in range(var_count):
                row = row_of(guest_star.at[group], v * var_count + w)
                chosen.append(jnp.where(lane % SUB == sublane, row, 0.0))
            out_rows = dot(both(chosen), picks)
            for w in range(var_count):
                at = 2 * SUB * w
                for i, s in enumerate(members):
                    for d in range(dims):
                        to = slice((i * dims + d) * LANES, (i * dims + d + 1) * LANES)
                        guest_star_coef[s, d, v * var_count + w] = (
                            out_rows[at : at + SUB, to]
                            + out_rows[at + SUB : at + 2 * SUB, to]
                        )
    guest_far, guest_index, guest_face = [], [], []
    for t in range(tiles):
        member = t * stack + sub_stack
        index = (member % per_group) * slots + sub_slot + block * j_block
        group = t * stack // per_group
        for pair in range(pairs):
            row = row_of(guest_plus.at[group], pair)
            guest_plus_coef[t, pair] = take(row, index)
        code = jnp.full((SUB, LANES), -1, jnp.int32)
        face = jnp.zeros((SUB, LANES), jnp.int32)
        spin = jnp.zeros((SUB, LANES), jnp.int32)
        for part in range(stack):
            k = t * stack + part
            if k < len(near):
                here = sub_stack == part
                got = take(row_of(early_in.at[k], deep), block * j_block + sub_slot)
                code = jnp.where(here, got.astype(jnp.int32), code)
                got = take(row_of(early_in.at[k], deep + 2), sub_slot)
                face = jnp.where(here, got.astype(jnp.int32), face)
                spin = jnp.where(here, near[k][1], spin)
        there = jnp.maximum(code, 0)
        step_delta = there // (n_sub * slots) - 1
        step_turn = lax.rem((there // slots) % n_sub + spin, n_sub)
        guest_index.append((there % slots) * j_block + inside)
        guest_far.append(jnp.where(code < 0, -1, (step_delta + 1) * n_sub + step_turn))
        guest_face.append(face * j_block + inside)

    def gather_far(sources, places, index, start):
        result = list(start)
        for v in range(var_count):
            for name, ref in sources:
                row = row_of(ref, v)
                result[v] = jnp.where(places == name, take(row, index), result[v])
        return result

    nothing = [jnp.zeros((SUB, LANES), F32)] * var_count
    for copy in first_copies:
        copy.wait_recv()
    far_weights = back_weights[dims * LANES :, :]
    own_sources = [
        (place(delta, turn), first_in.at[place(delta, turn)])
        for delta in (-1, 0, 1)
        for turn in range(n_sub)
        if delta or turn
    ]
    flux = [
        flux_of(
            plus_coef.at[h],
            gather_far(own_sources, far_place[h], far_index[h], nothing),
        )
        for h in range(halves)
    ]
    moved = [a + b for a, b in zip(partial, product(flux, far_weights))]
    guest_change = []
    for s in range(sets):
        flux = []
        for h in range(halves):
            t = s * halves + h
            if t < tiles:
                base = near[t * stack][0]
                sources = [
                    ((d + 1) * n_sub + turn, first_in.at[place(base + d, turn)])
                    for d in (-1, 0, 1)
                    for turn in range(n_sub)
                ]
                got = gather_far(sources, guest_far[t], guest_index[t], nothing)
                flux.append(flux_of(guest_plus_coef.at[t], got))
        guest_change.append(
            product(flux, back_weights[dims * LANES : (dims + len(flux)) * LANES, :])
        )

    for copy in near_copies:
        copy.wait_recv()
    guest_state = []
    for s in range(sets):
        states = []
        for v in range(var_count):
            value = guest_change[s][v]
            t, part = v // per_set, v % per_set
            for h in range(halves):
                for j in range(stack):
                    k = s * per_set + h * stack + j
                    if k < len(near):
                        got = near_in[k, t * SUB : (t + 1) * SUB, :]
                        if part % stack != j:
                            got = pltpu.roll(got, ((j - part % stack) * slots) % SUB, 0)
                        if part // stack != h:
                            got = pltpu.roll(
                                got, ((h - part // stack) * m_block) % LANES, 1
                            )
                        here = (sub_stack == j) & (mode_half == h)
                        value = jnp.where(here, value + got, value)
            states.append(value)
        guest_state.append(states)

    coefs = [star_coef] + [guest_star_coef.at[s] for s in range(sets)]
    current = [moved] + guest_state
    sums = [[first_weights[0] * tile for tile in value] for value in current]
    for term in range(1, ORDER):
        current = [step(coef, value) for coef, value in zip(coefs, current)]
        sums = [
            [a + first_weights[term] * b for a, b in zip(total, value)]
            for total, value in zip(sums, current)
        ]
    carried = [jnp.where(fine, a, b) for a, b in zip(sums[0], second_half)]
    values = face_values(carried)
    for s in range(sets):
        guest_values = face_values(sums[s + 1])
        for h in range(halves):
            t = s * halves + h
            if t < tiles:
                for v in range(var_count):
                    row = jnp.where(
                        block == sub_slot, take(guest_values[v][h], guest_face[t]), 0.0
                    )
                    for part in range(stack):
                        k = t * stack + part
                        if k < len(near):
                            one = jnp.sum(
                                row[part * slots : (part + 1) * slots],
                                axis=0,
                                keepdims=True,
                            )
                            at = nears * SUB + v
                            guest_rows[k, v : v + 1, :] = jnp.where(
                                early_in[k, deep + 1 : deep + 2, :] > 0.5,
                                one,
                                near_in[k, at : at + 1, :],
                            )
    last_sources = [
        (place(delta, turn), guest_rows.at[k]) for k, (delta, turn) in enumerate(near)
    ]
    beside = gather_local(values)
    flux = []
    for h in range(halves):
        got = gather_far(last_sources, far_place[h], far_index[h], beside[h])
        own = flux_of(minus_coef.at[h], [values[w][h] for w in range(var_count)])
        other = flux_of(plus_coef.at[h], got)
        flux.append([a + b for a, b in zip(own, other)])
    result = [
        a + b
        for a, b in zip(
            moved, product(mixed(star_coef, carried) + flux, back_weights[...])
        )
    ]
    for v in range(var_count):
        for h in range(halves):
            out[v, h * SUB : (h + 1) * SUB, :] = result[v][
                :, h * m_block : h * m_block + modes
            ]
    for copy in early_copies + first_copies + near_copies:
        copy.wait_send()


def solution(mesh):
    n_dom, n_sub = mesh.shape["dom"], mesh.shape["sub"]

    def per_device(
        dofs,
        stiffness,
        projection,
        star,
        flux_minus,
        flux_plus,
        fault_flux,
        fault_faces,
        levels,
        face_source,
        send_source,
    ):
        var_count, modes, elems = dofs.shape
        dims = stiffness.shape[0]
        faces, face_modes = projection.shape[0], projection.shape[1]
        halves = elems // SUB
        pairs = var_count * var_count
        slots = send_source.shape[0]
        quarters = max(faces, slots)
        j_block = LANES // quarters
        deep = up_to(-(-pairs // quarters), SUB)
        count = quarters * deep
        pitch = max(dims, faces)
        near, wide = 3 * n_sub - 1, 5 * n_sub - 1
        stack = SUB // slots
        tiles = -(-near // stack)
        sets = -(-tiles // halves)
        groups = -(-near // (j_block // slots))
        near_rows = -(-var_count // (stack * halves)) * SUB + var_count
        moved = [
            jnp.transpose(dofs, (0, 2, 1)),
            stiffness,
            jnp.transpose(projection, (1, 0, 2)),
            jnp.transpose(star, (1, 2, 0, 3)),
            jnp.transpose(flux_minus, (1, 2, 0, 3)),
            jnp.transpose(flux_plus, (1, 2, 0, 3)),
            fault_flux,
            fault_faces,
            levels.reshape(1, -1),
            face_source,
            send_source.reshape(1, -1),
        ]
        result = pl.pallas_call(
            functools.partial(kernel, (n_dom, n_sub)),
            out_shape=pltpu.VMEM((var_count, elems, modes), F32),
            in_specs=[pl.BlockSpec(memory_space=pltpu.HBM)] * len(moved),
            out_specs=pl.BlockSpec(memory_space=pltpu.VMEM),
            scratch_shapes=[pltpu.VMEM(one.shape, one.dtype) for one in moved]
            + [
                pltpu.VMEM((count * pitch, LANES), F32),
                pltpu.VMEM((count * pitch, LANES), F32),
                pltpu.VMEM((count * pitch, LANES), F32),
                pltpu.VMEM((count, LANES), F32),
                pltpu.VMEM((count, LANES), F32),
                pltpu.VMEM((count, LANES), F32),
                pltpu.VMEM((SUB, LANES), jnp.int32),
                pltpu.VMEM((LANES, LANES), F32),
                pltpu.VMEM((count, LANES), F32),
                pltpu.VMEM((dims, LANES, LANES), F32),
                pltpu.VMEM((halves * LANES, LANES), F32),
                pltpu.VMEM((dims, pairs, SUB, LANES), F32),
                pltpu.VMEM((halves, pairs, SUB, LANES), F32),
                pltpu.VMEM((halves, pairs, SUB, LANES), F32),
                pltpu.VMEM((dims * LANES, 2 * LANES), BF16),
                pltpu.VMEM(((dims + halves) * LANES, 2 * LANES), BF16),
                pltpu.VMEM((LANES, 2 * halves * LANES), BF16),
                pltpu.VMEM((var_count, halves, SUB, LANES), F32),
                pltpu.VMEM((var_count, SUB, LANES), F32),
                pltpu.VMEM((groups, count, LANES), F32),
                pltpu.VMEM((groups, count, LANES), F32),
                pltpu.VMEM((sets, dims, pairs, SUB, LANES), F32),
                pltpu.VMEM((tiles, pairs, SUB, LANES), F32),
                pltpu.VMEM((near, var_count, LANES), F32),
                pltpu.VMEM((deep + SUB, LANES), F32),
                pltpu.VMEM((near, deep + SUB, LANES), F32),
                pltpu.VMEM((near_rows, LANES), F32),
                pltpu.VMEM((near, near_rows, LANES), F32),
                pltpu.VMEM((var_count, LANES), F32),
                pltpu.VMEM((5 * n_sub, var_count, LANES), F32),
                pltpu.SemaphoreType.DMA((len(moved),)),
                pltpu.SemaphoreType.DMA((near,)),
                pltpu.SemaphoreType.DMA((near,)),
                pltpu.SemaphoreType.DMA((near,)),
                pltpu.SemaphoreType.DMA((near,)),
                pltpu.SemaphoreType.DMA((wide,)),
                pltpu.SemaphoreType.DMA((wide,)),
            ],
            compiler_params=pltpu.CompilerParams(
                collective_id=0,
                has_side_effects=True,
                vmem_limit_bytes=66_000_000,
            ),
            name="window",
        )(*moved)
        return jnp.transpose(result, (0, 2, 1))

    return jax.shard_map(
        per_device,
        mesh=mesh,
        in_specs=(
            P(None, None, ("dom", "sub")),
            P(),
            P(),
            P(None, None, None, ("dom", "sub")),
            P(None, None, None, ("dom", "sub")),
            P(None, None, None, ("dom", "sub")),
            P(),
            P(None, ("dom", "sub")),
            P(("dom", "sub")),
            P(None, ("dom", "sub")),
            P(("dom", "sub")),
        ),
        out_specs=P(None, None, ("dom", "sub")),
        check_vma=False,
    )
```

```python
import functools
import math

import jax
import jax.numpy as jnp
from jax import lax
from jax.experimental import pallas as pl
from jax.experimental.pallas import tpu as pltpu
from jax.sharding import PartitionSpec as P

MESH = pl.DeviceIdType.MESH
ORDER = 6
fine_step = 0.75
F32 = jnp.float32
BF16 = jnp.bfloat16
SUB = 8
LANES = 128


def taylor_weights(start_time, stop_time, term_count):
    return [
        (stop_time ** (term + 1) - start_time ** (term + 1)) / math.factorial(term + 1)
        for term in range(term_count)
    ]


def up_to(value, step):
    return -(-value // step) * step


def dot(a, b):
    return jnp.dot(a, b, preferred_element_type=F32)


def take(value, index):
    return jnp.take_along_axis(value, index, axis=1, mode="promise_in_bounds")


def total_of(parts):
    return functools.reduce(lambda a, b: a + b, parts)


def both(tiles):
    parts = []
    for tile in tiles:
        high = tile.astype(BF16).astype(F32)
        parts += [high, tile - high]
    return jnp.concatenate(parts, axis=0).astype(BF16)


def spread(rows, keep, picks):
    out = dot(both([jnp.where(keep, row, 0.0) for row in rows]), picks)
    blocks = picks.shape[1] // LANES
    return [
        [
            out[2 * SUB * i : 2 * SUB * i + SUB, b * LANES : (b + 1) * LANES]
            + out[2 * SUB * i + SUB : 2 * SUB * (i + 1), b * LANES : (b + 1) * LANES]
            for b in range(blocks)
        ]
        for i in range(len(rows))
    ]


def product(columns, weights):
    lhs = jnp.concatenate([both(tiles) for tiles in columns], axis=1)
    out = dot(lhs, weights)
    half = weights.shape[1] // 2
    result = []
    for v in range(len(columns[0])):
        at = 2 * SUB * v
        result.append(
            out[at : at + SUB, :half]
            + out[at : at + SUB, half:]
            + out[at + SUB : at + 2 * SUB, :half]
        )
    return result


def kernel(
    sizes,
    dofs_hbm,
    stiffness_hbm,
    projection_hbm,
    star_hbm,
    minus_hbm,
    plus_hbm,
    fault_hbm,
    fault_faces_hbm,
    levels_hbm,
    face_source_hbm,
    send_source_hbm,
    out,
    dofs,
    stiffness,
    projection,
    star,
    flux_minus,
    flux_plus,
    fault_flux,
    fault_faces,
    levels,
    face_source,
    send_source,
    star_lines,
    minus_lines,
    plus_lines,
    packed_star,
    packed_minus,
    packed_plus,
    ints,
    square,
    fault_rows,
    diagonal,
    spread_projection,
    star_coef,
    minus_coef,
    plus_coef,
    series_weights,
    back_weights,
    face_weights,
    faces_ref,
    part_ref,
    fine_ref,
    guest_star,
    guest_plus,
    guest_star_coef,
    guest_plus_coef,
    guest_rows,
    early_out,
    early_in,
    near_out,
    near_in,
    first_out,
    first_in,
    second_out,
    second_in,
    load_sem,
    early_send,
    early_recv,
    near_send,
    near_recv,
    first_send,
    first_recv,
    second_send,
    second_recv,
):
    n_dom, n_sub = sizes
    var_count, elems, modes = dofs.shape
    dims = stiffness.shape[0]
    face_modes, faces = projection.shape[0], projection.shape[1]
    slots = send_source.shape[1]
    halves = elems // SUB
    m_block = LANES // halves
    j_block = LANES // max(faces, slots)
    quarters = LANES // j_block
    pairs = var_count * var_count
    pitch = star_lines.shape[0] // packed_star.shape[0]
    deep = packed_star.shape[0] // quarters
    stack = SUB // slots
    per_set = stack * halves
    per_group = j_block // slots

    near = [
        (delta, turn)
        for delta in (1, -1, 0)
        for turn in reversed(range(n_sub))
        if delta or turn
    ]
    wide = [
        (delta, turn)
        for delta in (1, 2, -1, -2, 0)
        for turn in reversed(range(n_sub))
        if delta or turn
    ]
    followed = stack + len(near)
    tiles = -(-followed // stack)
    sets = -(-tiles // halves)

    def place(delta, turn):
        return (delta + 2) * n_sub + turn % n_sub

    loads = [
        pltpu.make_async_copy(src, dst, load_sem.at[i])
        for i, (src, dst) in enumerate(
            (
                (star_hbm, star),
                (stiffness_hbm, stiffness),
                (dofs_hbm, dofs),
                (projection_hbm, projection),
                (face_source_hbm, face_source),
                (send_source_hbm, send_source),
                (levels_hbm, levels),
                (fault_faces_hbm, fault_faces),
                (fault_hbm, fault_flux),
                (plus_hbm, flux_plus),
                (minus_hbm, flux_minus),
            )
        )
    ]
    for load in loads:
        load.start()

    me_dom, me_sub = lax.axis_index("dom"), lax.axis_index("sub")

    def device(delta, turn):
        return (
            lax.rem(me_dom + delta + n_dom, n_dom),
            lax.rem(me_sub + turn, n_sub),
        )

    barrier = pltpu.get_barrier_semaphore()
    for delta, turn in wide:
        pl.semaphore_signal(
            barrier, inc=1, device_id=device(delta, turn), device_id_type=MESH
        )

    diagonal[...] = jnp.zeros_like(diagonal)
    spread_projection[...] = jnp.zeros_like(spread_projection)
    ints[...] = jnp.zeros_like(ints)
    square[...] = jnp.zeros_like(square)

    sublane = lax.broadcasted_iota(jnp.int32, (SUB, LANES), 0)
    lane = lax.broadcasted_iota(jnp.int32, (SUB, LANES), 1)
    mode_half = lane // m_block
    block = lane // j_block
    inside = lane % j_block
    lane_slot = lane % slots
    sub_slot = sublane % slots
    sub_stack = sublane // slots
    star_index = mode_half * SUB + sublane
    flux_index = [block * j_block + h * SUB + sublane for h in range(halves)]

    def row_of(ref, at):
        return jnp.broadcast_to(ref[at : at + 1, :], (SUB, LANES))

    loads[0].wait()

    def lines(ref, source, count):
        for v in range(var_count):
            for w in range(var_count):
                at = (v * var_count + w) * pitch
                ref[at : at + count, 0:elems] = source[v, w]

    def pack(ref, count):
        depth = packed_star.shape[0]
        where = lax.broadcasted_iota(jnp.int32, (depth, LANES), 1) // j_block
        value = ref[pl.ds(0, depth, stride=pitch), :]
        for f in range(1, count):
            part = ref[pl.ds(f, depth, stride=pitch), :]
            value = jnp.where(where == f, pltpu.roll(part, f * j_block, 1), value)
        return value

    for load in loads[1:9]:
        load.wait()
    lines(star_lines, star, dims)
    packed_star[...] = pack(star_lines, dims)
    from_lane = lax.broadcasted_iota(jnp.int32, (LANES, LANES), 0)
    to_half = lax.broadcasted_iota(jnp.int32, (LANES, LANES), 1) // m_block
    keep = lane % SUB == sublane

    def picks_of(first, count):
        return jnp.concatenate(
            [
                jnp.where(
                    (from_lane // j_block == d)
                    & (from_lane % j_block // SUB == first + to_half),
                    1.0,
                    0.0,
                )
                for d in range(count)
            ],
            axis=1,
        ).astype(BF16)

    by_matmul = min(dims, 2)
    own_picks = picks_of(0, by_matmul)
    for v in range(var_count):
        at = v * var_count
        rows = [row_of(packed_star, at + w) for w in range(var_count)]
        for w, tiles_of in enumerate(spread(rows, keep, own_picks)):
            for d, tile in enumerate(tiles_of):
                star_coef[d, at + w] = tile
    for d in range(by_matmul, dims):
        for pair in range(pairs):
            star_coef[d, pair] = take(row_of(star_lines, pair * pitch + d), star_index)

    for d in range(dims):
        for h in range(halves):
            at = slice(h * m_block, h * m_block + modes)
            diagonal[d, at, at] = stiffness[d]

    def put(ref, at, value):
        high = value.astype(BF16)
        count, width = value.shape
        ref[at : at + count, 0:width] = high
        ref[at : at + count, width : 2 * width] = (value - high.astype(F32)).astype(BF16)

    for d in range(dims):
        put(series_weights, d * LANES, jnp.transpose(diagonal[d]))

    state = []
    for v in range(var_count):
        parts = []
        for h in range(halves):
            parts.append(dofs[v, h * SUB : (h + 1) * SUB, :])
            if m_block > modes:
                parts.append(jnp.zeros((SUB, m_block - modes), F32))
        state.append(jnp.concatenate(parts, axis=1))

    def mixed(coef, value):
        return [
            [
                total_of(
                    [coef[d, v * var_count + w] * value[w] for w in range(var_count)]
                )
                for v in range(var_count)
            ]
            for d in range(dims)
        ]

    def step(coef, value):
        return product(mixed(coef, value), series_weights[...])

    first_weights = taylor_weights(0.0, fine_step, ORDER)
    second_weights = taylor_weights(fine_step, 2.0 * fine_step, ORDER)

    for h in range(halves):
        for f in range(faces):
            at = h * LANES + f * j_block
            spread_projection[
                at : at + face_modes, h * m_block : h * m_block + modes
            ] = projection[:, f, :]
    put(face_weights, 0, jnp.transpose(spread_projection[...]))
    for d in range(dims):
        put(back_weights, d * LANES, diagonal[d])
    put(back_weights, dims * LANES, -spread_projection[...])

    for f in range(faces):
        at = slice(f * j_block, f * j_block + elems)
        ints[0:1, at] = face_source[f : f + 1, :]
        ints[1:2, at] = fault_faces[f : f + 1, :]
    ints[2:3, 0:elems] = levels[...]
    ints[3:4, 0:slots] = send_source[...]

    raw = row_of(ints, 0)
    beyond = jnp.maximum(raw - faces * elems, 0)
    code_delta = beyond // (n_sub * slots) - 1
    code_turn = lax.rem((beyond // slots) % n_sub - me_sub + n_sub, n_sub)
    code_slot = beyond % slots
    own_export = take(row_of(ints, 3), code_slot)
    is_far = raw >= faces * elems
    is_own = is_far & (code_delta == 0) & (code_turn == 0)
    local_code = jnp.where(is_own, own_export, jnp.where(is_far, -1, raw))
    far_code = jnp.where(
        is_far & jnp.logical_not(is_own),
        ((code_delta + 1) * n_sub + code_turn) * slots + code_slot,
        -1,
    )
    local_index, local_elem, far_index, far_place = [], [], [], []
    for h in range(halves):
        local = take(local_code, flux_index[h])
        far = take(far_code, flux_index[h])
        near_by = jnp.maximum(local, 0)
        there = jnp.maximum(far, 0)
        local_index.append((near_by // elems) * j_block + inside)
        local_elem.append(jnp.where(local < 0, -1, near_by % elems))
        far_index.append((there % slots) * j_block + inside)
        far_place.append(jnp.where(far < 0, -1, there // slots + n_sub))
    sent = take(row_of(ints, 3), block)
    sent_index = (sent // elems) * j_block + inside
    sent_elem = sent % elems
    small = take(row_of(ints, 3), lane_slot)
    small_elem = small % elems
    rising = take(row_of(ints, 3), sub_slot) % elems

    square[0:var_count, 0:var_count] = fault_flux[...]
    turned = jnp.transpose(square[...])[0 : up_to(var_count, SUB)]
    for v in range(var_count):
        column = jnp.broadcast_to(turned[:, v : v + 1], (turned.shape[0], LANES))
        fault_rows[v * var_count : (v + 1) * var_count, :] = column[0:var_count]
    loads[9].wait()
    lines(plus_lines, flux_plus, faces)
    on_fault = jnp.broadcast_to(ints[1:2, :], packed_plus.shape) == 1
    packed_plus[...] = jnp.where(on_fault, fault_rows[...], pack(plus_lines, faces))

    part_of = inside // slots
    early_star = jnp.minimum(part_of, dims - 1) * j_block + small_elem
    early_plus = jnp.clip(part_of - dims, 0, faces - 1) * j_block + small_elem
    for i in range(deep // SUB):
        value = jnp.zeros((SUB, LANES), F32)
        for q in range(quarters):
            at = slice(q * deep + i * SUB, q * deep + (i + 1) * SUB)
            one = jnp.where(
                part_of < dims,
                take(packed_star[at, :], early_star),
                take(packed_plus[at, :], early_plus),
            )
            value = jnp.where(block == q, one, value)
        early_out[i * SUB : (i + 1) * SUB, :] = value
    marks = [
        take(far_code, block * j_block + small_elem),
        jnp.where(take(row_of(ints, 2), sent_elem) == 0, 1, 0),
        small // elems,
    ]
    for i, mark in enumerate(marks):
        early_out[deep + i : deep + i + 1, :] = mark[0:1].astype(F32)

    def send(source, target, partners, index_of, send_sem, recv_sem):
        for delta, turn in partners:
            pltpu.make_async_remote_copy(
                src_ref=source,
                dst_ref=target(index_of(-delta, -turn % n_sub)),
                send_sem=send_sem.at[0],
                recv_sem=recv_sem.at[0],
                device_id=device(delta, turn),
                device_id_type=MESH,
            ).start()

    def settle(whole, sem):
        pltpu.make_async_copy(whole, whole, sem.at[0]).wait()

    def near_place(delta, turn):
        return near.index((delta, turn))

    early_at = 2
    value, firsts = state, [first_weights[0] * tile for tile in state]
    seconds = [second_weights[0] * tile for tile in state]
    for term in range(1, ORDER):
        if term == early_at:
            pl.semaphore_wait(barrier, len(wide))
            send(
                early_out,
                lambda at: early_in.at[at],
                near,
                near_place,
                early_send,
                early_recv,
            )
            loads[10].wait()
            lines(minus_lines, flux_minus, faces)
            packed_minus[...] = pack(minus_lines, faces)
            for pair in range(pairs):
                row = row_of(packed_minus, pair)
                for h in range(halves):
                    minus_coef[h, pair] = take(row, flux_index[h])
            for pair in range(pairs):
                row = row_of(packed_plus, pair)
                for h in range(halves):
                    plus_coef[h, pair] = take(row, flux_index[h])
        value = step(star_coef, value)
        firsts = [a + first_weights[term] * b for a, b in zip(firsts, value)]
        seconds = [a + second_weights[term] * b for a, b in zip(seconds, value)]
    first_half, second_half = firsts, seconds

    def face_values(value):
        broad = product([value], face_weights[...])
        return [
            [tile[:, h * LANES : (h + 1) * LANES] for h in range(halves)]
            for tile in broad
        ]

    def export(ref, at, values):
        for v in range(var_count):
            picked = total_of(
                [
                    jnp.where(
                        sent_elem == h * SUB + sublane, take(values[v][h], sent_index), 0.0
                    )
                    for h in range(halves)
                ]
            )
            ref[at + v : at + v + 1, :] = jnp.sum(picked, axis=0, keepdims=True)

    def flux_of(coef, values):
        return [
            total_of([coef[v * var_count + w] * values[w] for w in range(var_count)])
            for v in range(var_count)
        ]

    def gather_shifted(rows, maps):
        result = []
        for shifts in maps:
            parts = []
            for turn, source in enumerate(shifts):
                one = jnp.where(source == 0, rows[0], 0.0)
                for at in range(1, len(rows)):
                    one = jnp.where(source == at, rows[at], one)
                parts.append(pltpu.roll(one, turn * j_block, 1) if turn else one)
            result.append(total_of(parts))
        return result

    def gather_local(values, elem_map):
        for v in range(var_count):
            for h in range(halves):
                faces_ref[v, h] = values[v][h]
        beside = [[jnp.zeros((SUB, LANES), F32)] * var_count for _ in range(halves)]
        for h in range(halves):
            for v in range(var_count):
                for e in range(elems):
                    row = row_of(faces_ref.at[v, e // SUB], e % SUB)
                    beside[h][v] = jnp.where(
                        elem_map[h] == e, take(row, local_index[h]), beside[h][v]
                    )
        return beside

    values = face_values(first_half)
    export(first_out, 0, values)
    send(
        first_out, lambda at: first_in.at[at], wide, place, first_send, first_recv
    )
    own_place = place(0, 0)
    first_in[own_place] = first_out[...]

    volume = product(mixed(star_coef, first_half), back_weights[0 : dims * LANES, :])
    beside = gather_local(values, local_elem)
    flux = []
    for h in range(halves):
        own = flux_of(minus_coef.at[h], [values[w][h] for w in range(var_count)])
        other = flux_of(plus_coef.at[h], beside[h])
        flux.append([a + b for a, b in zip(own, other)])
    partial = [
        a + b + c
        for a, b, c in zip(
            state, volume, product(flux, back_weights[dims * LANES :, :])
        )
    ]

    for v in range(var_count):
        part_ref[v] = partial[v]
    def pulled(elem):
        result = []
        for v in range(var_count):
            row = jnp.zeros((SUB, LANES), F32)
            for e in range(SUB):
                row = jnp.where(elem % SUB == e, row_of(part_ref.at[v], e), row)
            one = row
            for turn in range(1, halves):
                moved_row = pltpu.roll(row, turn * m_block, 1)
                one = jnp.where((elem // SUB + turn) % halves == mode_half, moved_row, one)
            result.append(one)
        return result

    nears = -(-var_count // per_set)
    rising_state = pulled(rising)
    for t in range(nears):
        value = jnp.zeros((SUB, LANES), F32)
        for part in range(per_set):
            v = t * per_set + part
            if v < var_count:
                here = (sub_stack == part % stack) & (mode_half == part // stack)
                value = jnp.where(here, rising_state[v], value)
        near_out[t * SUB : (t + 1) * SUB, :] = value
    last_parts = min(var_count - (nears - 1) * per_set, stack)
    near_rows = (nears - 1) * SUB + last_parts * slots
    send(
        near_out.at[0:near_rows],
        lambda at: near_in.at[at, 0:near_rows],
        near,
        near_place,
        near_send,
        near_recv,
    )
    second_values = face_values(second_half)
    export(second_out, 0, second_values)
    send(
        second_out,
        lambda at: second_in.at[at],
        near,
        near_place,
        second_send,
        second_recv,
    )
    is_fine = (row_of(ints, 2) == 0) & (lane < elems)
    below = lax.broadcasted_iota(jnp.int32, (LANES, LANES), 1)
    flags = jnp.where(is_fine, 1.0, 0.0)
    rank = dot(
        jnp.concatenate([flags, flags], axis=0).astype(BF16),
        jnp.where(from_lane < below, 1.0, 0.0).astype(BF16),
    )[0:SUB].astype(jnp.int32)
    fine_rank = jnp.where(is_fine, rank, -1)
    fine_elem = jnp.sum(
        jnp.where(fine_rank == sublane, lane.astype(F32), 0.0), axis=1, keepdims=True
    )
    fine_elem = jnp.broadcast_to(fine_elem, (SUB, LANES))
    fine_across = jnp.sum(jnp.where(keep, fine_elem, 0.0), axis=0, keepdims=True)
    fine_across = jnp.broadcast_to(fine_across, (SUB, LANES)).astype(jnp.int32)
    fine_elem = fine_elem.astype(jnp.int32)
    home = take(fine_rank, star_index)
    local_rank, coarse_elem = [], []
    for h in range(halves):
        source = take(fine_rank, jnp.maximum(local_elem[h], 0))
        local_rank.append(jnp.where(local_elem[h] < 0, -1, source))
        coarse_elem.append(jnp.where(local_rank[h] < 0, local_elem[h], -1))

    def shifted(index, elem):
        result = []
        for turn in range(quarters):
            away = (block - index // j_block + quarters) % quarters
            kept = jnp.where(away == turn, elem, -1)
            result.append(
                pltpu.roll(kept, (quarters - turn) % quarters * j_block, 1)
                if turn
                else kept
            )
        return result

    rank_shift = [shifted(a, b) for a, b in zip(local_index, local_rank)]

    own_state = pulled(fine_elem)
    coarse_beside = gather_local(second_values, coarse_elem)

    settle(early_in, early_recv)
    groups = -(-followed // per_group)
    for group in range(groups):
        members = range(group * per_group, min(followed, (group + 1) * per_group))
        for q in range(quarters):
            star_from = q * j_block + jnp.minimum(block, dims - 1) * slots + lane_slot
            plus_from = q * j_block + (dims + jnp.minimum(block, faces - 1)) * slots + lane_slot
            for i in range(deep // SUB):
                at = slice(q * deep + i * SUB, q * deep + (i + 1) * SUB)
                one = jnp.zeros((SUB, LANES), F32)
                two = one
                if group == 0:
                    here = part_of < stack
                    own = jnp.minimum(block, dims - 1) * j_block + fine_across
                    one = jnp.where(here, take(packed_star[at, :], own), one)
                    own = jnp.minimum(block, faces - 1) * j_block + fine_across
                    two = jnp.where(here, take(packed_plus[at, :], own), two)
                for k in members:
                    if k < stack:
                        continue
                    got = early_in[k - stack, i * SUB : (i + 1) * SUB, :]
                    here = part_of == k % per_group
                    one = jnp.where(here, take(got, star_from), one)
                    two = jnp.where(here, take(got, plus_from), two)
                guest_star[group, at, :] = one
                guest_plus[group, at, :] = two
    for group in range(groups):
        members = [s for s in range(sets) if s * per_set // per_group == group]
        picks = jnp.concatenate(
            [picks_of(s * per_set % per_group // stack, dims) for s in members], axis=1
        )
        for v in range(var_count):
            at = v * var_count
            rows = [row_of(guest_star.at[group], at + w) for w in range(var_count)]
            for w, tiles_of in enumerate(spread(rows, keep, picks)):
                for i, tile in enumerate(tiles_of):
                    guest_star_coef[members[i // dims], i % dims, at + w] = tile
    guest_far, guest_index, guest_face = [], [], []
    for t in range(tiles):
        member = t * stack + sub_stack
        index = (member % per_group) * slots + sub_slot + block * j_block
        group = t * stack // per_group
        for pair in range(pairs):
            row = row_of(guest_plus.at[group], pair)
            guest_plus_coef[t, pair] = take(row, index)
        code = jnp.full((SUB, LANES), -1, jnp.int32)
        face = jnp.zeros((SUB, LANES), jnp.int32)
        spin = jnp.zeros((SUB, LANES), jnp.int32)
        if t == 0:
            code = take(far_code, block * j_block + fine_elem)
        for part in range(stack):
            k = (t - 1) * stack + part
            if 0 <= k < len(near):
                here = sub_stack == part
                got = take(row_of(early_in.at[k], deep), block * j_block + sub_slot)
                code = jnp.where(here, got.astype(jnp.int32), code)
                got = take(row_of(early_in.at[k], deep + 2), sub_slot)
                face = jnp.where(here, got.astype(jnp.int32), face)
                spin = jnp.where(here, near[k][1], spin)
        there = jnp.maximum(code, 0)
        step_delta = there // (n_sub * slots) - 1
        step_turn = lax.rem((there // slots) % n_sub + spin, n_sub)
        guest_index.append((there % slots) * j_block + inside)
        guest_far.append(jnp.where(code < 0, -1, (step_delta + 1) * n_sub + step_turn))
        guest_face.append(face * j_block + inside)

    def gather_far(sources, places, index, start):
        result = list(start)
        for v in range(var_count):
            for name, ref in sources:
                row = row_of(ref, v)
                result[v] = jnp.where(places == name, take(row, index), result[v])
        return result

    nothing = [jnp.zeros((SUB, LANES), F32)] * var_count
    settle(first_in.at[0 : len(wide)], first_recv)
    far_weights = back_weights[dims * LANES :, :]
    guest_change = []
    for s in range(sets):
        flux = []
        for h in range(halves):
            t = s * halves + h
            if t < tiles:
                base = near[(t - 1) * stack][0] if t else 0
                sources = [
                    ((d + 1) * n_sub + turn, first_in.at[place(base + d, turn)])
                    for d in (-1, 0, 1)
                    for turn in range(n_sub)
                ]
                got = gather_far(sources, guest_far[t], guest_index[t], nothing)
                flux.append(flux_of(guest_plus_coef.at[t], got))
        guest_change.append(
            product(flux, back_weights[dims * LANES : (dims + len(flux)) * LANES, :])
        )

    settle(near_in.at[:, 0:near_rows], near_recv)
    settle(second_in, second_recv)
    guest_state = []
    for s in range(sets):
        states = []
        for v in range(var_count):
            value = guest_change[s][v]
            t, part = v // per_set, v % per_set
            for h in range(halves):
                if s == 0 and h == 0:
                    value = jnp.where(mode_half == 0, value + own_state[v], value)
                    continue
                for j in range(stack):
                    k = s * per_set + (h - 1) * stack + j
                    if k < len(near):
                        got = near_in[k, t * SUB : (t + 1) * SUB, :]
                        if part % stack != j:
                            got = pltpu.roll(got, ((j - part % stack) * slots) % SUB, 0)
                        if part // stack != h:
                            got = pltpu.roll(
                                got, ((h - part // stack) * m_block) % LANES, 1
                            )
                        here = (sub_stack == j) & (mode_half == h)
                        value = jnp.where(here, value + got, value)
            states.append(value)
        guest_state.append(states)

    coefs = [guest_star_coef.at[s] for s in range(sets)]
    current = guest_state
    sums = [[first_weights[0] * tile for tile in value] for value in current]
    for term in range(1, ORDER):
        current = [step(coef, value) for coef, value in zip(coefs, current)]
        sums = [
            [a + first_weights[term] * b for a, b in zip(total, value)]
            for total, value in zip(sums, current)
        ]
    own_sources = [
        (place(delta, turn), first_in.at[place(delta, turn)])
        for delta in (-1, 0, 1)
        for turn in range(n_sub)
        if delta or turn
    ]
    flux = [
        flux_of(
            plus_coef.at[h],
            gather_far(own_sources, far_place[h], far_index[h], nothing),
        )
        for h in range(halves)
    ]
    moved = [a + b for a, b in zip(partial, product(flux, far_weights))]
    coarse_far, guest_at = [], []
    marks = [
        (place(delta, turn), early_in.at[k, deep + 1 : deep + 2])
        for k, (delta, turn) in enumerate(near)
    ]
    last_sources = [
        (place(delta, turn), second_in.at[k]) for k, (delta, turn) in enumerate(near)
    ]
    for h in range(halves):
        coarse_far.append(
            gather_far(last_sources, far_place[h], far_index[h], coarse_beside[h])
        )
        mark = jnp.zeros((SUB, LANES), F32)
        code = jnp.full((SUB, LANES), -1, jnp.int32)
        for k, (name, ref) in enumerate(marks):
            here = far_place[h] == name
            mark = jnp.where(here, take(row_of(ref, 0), far_index[h]), mark)
            code = jnp.where(here, k * slots + far_index[h] // j_block, code)
        guest_at.append(jnp.where(mark > 0.5, code, -1))

    guest_values = [face_values(total) for total in sums]
    for v in range(var_count):
        fine_ref[v] = guest_values[0][v][0]
    carried = []
    for v in range(var_count):
        one = sums[0][v]
        for h in range(1, halves):
            one = jnp.where(mode_half == h, pltpu.roll(sums[0][v], h * m_block, 1), one)
        part_ref[v] = one
        one = second_half[v]
        for rank_at in range(SUB):
            one = jnp.where(home == rank_at, row_of(part_ref.at[v], rank_at), one)
        carried.append(one)
    values = face_values(carried)
    for s in range(sets):
        for h in range(halves):
            t = s * halves + h
            if 0 < t < tiles:
                for v in range(var_count):
                    guest_rows[t - 1, v] = take(guest_values[s][v][h], guest_face[t])
    fine_beside = []
    for v in range(var_count):
        rows = [row_of(fine_ref.at[v], at) for at in range(SUB)]
        fine_beside.append(gather_shifted(rows, rank_shift))
    volume = product(mixed(star_coef, carried), back_weights[0 : dims * LANES, :])
    flux = []
    for h in range(halves):
        got = []
        for v in range(var_count):
            one = coarse_far[h][v] + fine_beside[v][h]
            for at in range(len(near) * slots):
                row = row_of(guest_rows.at[at // SUB, v], at % SUB)
                one = jnp.where(guest_at[h] == at, row, one)
            got.append(one)
        own = flux_of(minus_coef.at[h], [values[w][h] for w in range(var_count)])
        other = flux_of(plus_coef.at[h], got)
        flux.append([a + b for a, b in zip(own, other)])
    result = [
        a + b + c
        for a, b, c in zip(
            moved, volume, product(flux, back_weights[dims * LANES :, :])
        )
    ]
    for v in range(var_count):
        for h in range(halves):
            out[v, h * SUB : (h + 1) * SUB, :] = result[v][
                :, h * m_block : h * m_block + modes
            ]
    settle(early_in, early_send)
    settle(first_in.at[0 : len(wide)], first_send)
    settle(second_in, second_send)
    settle(near_in.at[:, 0:near_rows], near_send)


def solution(mesh):
    n_dom, n_sub = mesh.shape["dom"], mesh.shape["sub"]

    def per_device(
        dofs,
        stiffness,
        projection,
        star,
        flux_minus,
        flux_plus,
        fault_flux,
        fault_faces,
        levels,
        face_source,
        send_source,
    ):
        var_count, modes, elems = dofs.shape
        dims = stiffness.shape[0]
        faces, face_modes = projection.shape[0], projection.shape[1]
        halves = elems // SUB
        pairs = var_count * var_count
        slots = send_source.shape[0]
        quarters = max(faces, slots)
        j_block = LANES // quarters
        deep = up_to(-(-pairs // quarters), SUB)
        count = quarters * deep
        pitch = max(dims, faces)
        near, wide = 3 * n_sub - 1, 5 * n_sub - 1
        stack = SUB // slots
        tiles = -(-(stack + near) // stack)
        sets = -(-tiles // halves)
        groups = -(-(stack + near) // (j_block // slots))
        near_rows = -(-var_count // (stack * halves)) * SUB
        moved = [
            jnp.transpose(dofs, (0, 2, 1)),
            stiffness,
            jnp.transpose(projection, (1, 0, 2)),
            jnp.transpose(star, (1, 2, 0, 3)),
            jnp.transpose(flux_minus, (1, 2, 0, 3)),
            jnp.transpose(flux_plus, (1, 2, 0, 3)),
            fault_flux,
            fault_faces,
            levels.reshape(1, -1),
            face_source,
            send_source.reshape(1, -1),
        ]
        result = pl.pallas_call(
            functools.partial(kernel, (n_dom, n_sub)),
            out_shape=pltpu.VMEM((var_count, elems, modes), F32),
            in_specs=[pl.BlockSpec(memory_space=pltpu.HBM)] * len(moved),
            out_specs=pl.BlockSpec(memory_space=pltpu.VMEM),
            scratch_shapes=[pltpu.VMEM(one.shape, one.dtype) for one in moved]
            + [
                pltpu.VMEM((count * pitch, LANES), F32),
                pltpu.VMEM((count * pitch, LANES), F32),
                pltpu.VMEM((count * pitch, LANES), F32),
                pltpu.VMEM((count, LANES), F32),
                pltpu.VMEM((count, LANES), F32),
                pltpu.VMEM((count, LANES), F32),
                pltpu.VMEM((SUB, LANES), jnp.int32),
                pltpu.VMEM((LANES, LANES), F32),
                pltpu.VMEM((count, LANES), F32),
                pltpu.VMEM((dims, LANES, LANES), F32),
                pltpu.VMEM((halves * LANES, LANES), F32),
                pltpu.VMEM((dims, pairs, SUB, LANES), F32),
                pltpu.VMEM((halves, pairs, SUB, LANES), F32),
                pltpu.VMEM((halves, pairs, SUB, LANES), F32),
                pltpu.VMEM((dims * LANES, 2 * LANES), BF16),
                pltpu.VMEM(((dims + halves) * LANES, 2 * LANES), BF16),
                pltpu.VMEM((LANES, 2 * halves * LANES), BF16),
                pltpu.VMEM((var_count, halves, SUB, LANES), F32),
                pltpu.VMEM((var_count, SUB, LANES), F32),
                pltpu.VMEM((var_count, SUB, LANES), F32),
                pltpu.VMEM((groups, count, LANES), F32),
                pltpu.VMEM((groups, count, LANES), F32),
                pltpu.VMEM((sets, dims, pairs, SUB, LANES), F32),
                pltpu.VMEM((tiles, pairs, SUB, LANES), F32),
                pltpu.VMEM((tiles - 1, var_count, SUB, LANES), F32),
                pltpu.VMEM((deep + SUB, LANES), F32),
                pltpu.VMEM((near, deep + SUB, LANES), F32),
                pltpu.VMEM((near_rows, LANES), F32),
                pltpu.VMEM((near, near_rows, LANES), F32),
                pltpu.VMEM((var_count, LANES), F32),
                pltpu.VMEM((5 * n_sub, var_count, LANES), F32),
                pltpu.VMEM((var_count, LANES), F32),
                pltpu.VMEM((near, var_count, LANES), F32),
                pltpu.SemaphoreType.DMA((len(moved),)),
            ]
            + [pltpu.SemaphoreType.DMA((1,))] * 8,
            compiler_params=pltpu.CompilerParams(
                collective_id=0,
                has_side_effects=True,
                vmem_limit_bytes=66_000_000,
            ),
            name="window",
        )(*moved)
        return jnp.transpose(result, (0, 2, 1))

    return jax.shard_map(
        per_device,
        mesh=mesh,
        in_specs=(
            P(None, None, ("dom", "sub")),
            P(),
            P(),
            P(None, None, None, ("dom", "sub")),
            P(None, None, None, ("dom", "sub")),
            P(None, None, None, ("dom", "sub")),
            P(),
            P(None, ("dom", "sub")),
            P(("dom", "sub")),
            P(None, ("dom", "sub")),
            P(("dom", "sub")),
        ),
        out_specs=P(None, None, ("dom", "sub")),
        check_vma=False,
    )
```

```python
import functools
import math

import jax
import jax.numpy as jnp
from jax import lax
from jax.experimental import pallas as pl
from jax.experimental.pallas import tpu as pltpu
from jax.sharding import PartitionSpec as P

MESH = pl.DeviceIdType.MESH
ORDER = 6
fine_step = 0.75
F32 = jnp.float32
BF16 = jnp.bfloat16
SUB = 8
LANES = 128
BY_TAKE = 4


def taylor_weights(start_time, stop_time, term_count):
    return [
        (stop_time ** (term + 1) - start_time ** (term + 1)) / math.factorial(term + 1)
        for term in range(term_count)
    ]


def up_to(value, step):
    return -(-value // step) * step


def dot(a, b):
    return jnp.dot(a, b, preferred_element_type=F32)


def take(value, index):
    return jnp.take_along_axis(value, index, axis=1, mode="promise_in_bounds")


def total_of(parts):
    return functools.reduce(lambda a, b: a + b, parts)


def both(tiles):
    parts = []
    for tile in tiles:
        high = tile.astype(BF16).astype(F32)
        parts += [high, tile - high]
    return jnp.concatenate(parts, axis=0).astype(BF16)


def spread(rows, keep, picks):
    out = dot(both([jnp.where(keep, row, 0.0) for row in rows]), picks)
    blocks = picks.shape[1] // LANES
    return [
        [
            out[2 * SUB * i : 2 * SUB * i + SUB, b * LANES : (b + 1) * LANES]
            + out[2 * SUB * i + SUB : 2 * SUB * (i + 1), b * LANES : (b + 1) * LANES]
            for b in range(blocks)
        ]
        for i in range(len(rows))
    ]


def product(columns, weights):
    lhs = jnp.concatenate([both(tiles) for tiles in columns], axis=1)
    out = dot(lhs, weights)
    half = weights.shape[1] // 2
    result = []
    for v in range(len(columns[0])):
        at = 2 * SUB * v
        result.append(
            out[at : at + SUB, :half]
            + out[at : at + SUB, half:]
            + out[at + SUB : at + 2 * SUB, :half]
        )
    return result


def kernel(
    sizes,
    dofs_hbm,
    stiffness_hbm,
    projection_hbm,
    star_hbm,
    minus_hbm,
    plus_hbm,
    fault_hbm,
    fault_faces_hbm,
    levels_hbm,
    face_source_hbm,
    send_source_hbm,
    out,
    dofs,
    stiffness,
    projection,
    star,
    flux_minus,
    flux_plus,
    fault_flux,
    fault_faces,
    levels,
    face_source,
    send_source,
    star_lines,
    minus_lines,
    plus_lines,
    packed_star,
    packed_minus,
    packed_plus,
    ints,
    square,
    fault_rows,
    diagonal,
    spread_projection,
    star_coef,
    minus_coef,
    plus_coef,
    series_weights,
    back_weights,
    face_weights,
    faces_ref,
    part_ref,
    fine_ref,
    exported_coef,
    both_weights,
    guest_star,
    guest_plus,
    guest_star_coef,
    guest_plus_coef,
    guest_rows,
    early_out,
    early_in,
    near_out,
    near_in,
    first_out,
    first_in,
    second_out,
    second_in,
    load_sem,
    early_send,
    early_recv,
    near_send,
    near_recv,
    first_send,
    first_recv,
    second_send,
    second_recv,
):
    n_dom, n_sub = sizes
    var_count, elems, modes = dofs.shape
    dims = stiffness.shape[0]
    face_modes, faces = projection.shape[0], projection.shape[1]
    slots = send_source.shape[1]
    halves = elems // SUB
    m_block = LANES // halves
    j_block = LANES // max(faces, slots)
    quarters = LANES // j_block
    pairs = var_count * var_count
    pitch = star_lines.shape[0] // packed_star.shape[0]
    deep = packed_star.shape[0] // quarters
    stack = SUB // slots
    per_set = stack * halves
    per_group = j_block // slots

    near = [
        (delta, turn)
        for delta in (1, -1, 0)
        for turn in reversed(range(n_sub))
        if delta or turn
    ]
    wide = [
        (delta, turn)
        for delta in (1, 2, -1, -2, 0)
        for turn in reversed(range(n_sub))
        if delta or turn
    ]
    followed = stack + len(near)
    tiles = -(-followed // stack)
    sets = -(-tiles // halves)

    def place(delta, turn):
        return (delta + 2) * n_sub + turn % n_sub

    loads = [
        pltpu.make_async_copy(src, dst, load_sem.at[i])
        for i, (src, dst) in enumerate(
            (
                (star_hbm, star),
                (stiffness_hbm, stiffness),
                (dofs_hbm, dofs),
                (projection_hbm, projection),
                (face_source_hbm, face_source),
                (send_source_hbm, send_source),
                (levels_hbm, levels),
                (fault_faces_hbm, fault_faces),
                (fault_hbm, fault_flux),
                (plus_hbm, flux_plus),
                (minus_hbm, flux_minus),
            )
        )
    ]
    for load in loads:
        load.start()

    me_dom, me_sub = lax.axis_index("dom"), lax.axis_index("sub")

    def device(delta, turn):
        return (
            lax.rem(me_dom + delta + n_dom, n_dom),
            lax.rem(me_sub + turn, n_sub),
        )

    barrier = pltpu.get_barrier_semaphore()
    for delta, turn in wide:
        pl.semaphore_signal(
            barrier, inc=1, device_id=device(delta, turn), device_id_type=MESH
        )

    diagonal[...] = jnp.zeros_like(diagonal)
    spread_projection[...] = jnp.zeros_like(spread_projection)
    ints[...] = jnp.zeros_like(ints)
    square[...] = jnp.zeros_like(square)

    sublane = lax.broadcasted_iota(jnp.int32, (SUB, LANES), 0)
    lane = lax.broadcasted_iota(jnp.int32, (SUB, LANES), 1)
    mode_half = lane // m_block
    block = lane // j_block
    inside = lane % j_block
    lane_slot = lane % slots
    sub_slot = sublane % slots
    sub_stack = sublane // slots
    star_index = mode_half * SUB + sublane
    flux_index = [block * j_block + h * SUB + sublane for h in range(halves)]

    def row_of(ref, at):
        return jnp.broadcast_to(ref[at : at + 1, :], (SUB, LANES))

    loads[0].wait()

    def lines(ref, source, count):
        for v in range(var_count):
            for w in range(var_count):
                at = (v * var_count + w) * pitch
                ref[at : at + count, 0:elems] = source[v, w]

    def pack(ref, count):
        depth = packed_star.shape[0]
        where = lax.broadcasted_iota(jnp.int32, (depth, LANES), 1) // j_block
        value = ref[pl.ds(0, depth, stride=pitch), :]
        for f in range(1, count):
            part = ref[pl.ds(f, depth, stride=pitch), :]
            value = jnp.where(where == f, pltpu.roll(part, f * j_block, 1), value)
        return value

    for load in loads[1:9]:
        load.wait()
    lines(star_lines, star, dims)
    packed_star[...] = pack(star_lines, dims)
    from_lane = lax.broadcasted_iota(jnp.int32, (LANES, LANES), 0)
    to_half = lax.broadcasted_iota(jnp.int32, (LANES, LANES), 1) // m_block
    keep = lane % SUB == sublane

    def picks_of(first, count):
        return jnp.concatenate(
            [
                jnp.where(
                    (from_lane // j_block == d)
                    & (from_lane % j_block // SUB == first + to_half),
                    1.0,
                    0.0,
                )
                for d in range(count)
            ],
            axis=1,
        ).astype(BF16)

    by_matmul = min(dims, 2)
    own_picks = picks_of(0, by_matmul)
    for v in range(var_count):
        at = v * var_count
        rows = [row_of(packed_star, at + w) for w in range(var_count)]
        for w, tiles_of in enumerate(spread(rows, keep, own_picks)):
            for d, tile in enumerate(tiles_of):
                star_coef[d, at + w] = tile
    for d in range(by_matmul, dims):
        for pair in range(pairs):
            star_coef[d, pair] = take(row_of(star_lines, pair * pitch + d), star_index)

    for d in range(dims):
        for h in range(halves):
            at = slice(h * m_block, h * m_block + modes)
            diagonal[d, at, at] = stiffness[d]

    def put(ref, at, value):
        high = value.astype(BF16)
        count, width = value.shape
        ref[at : at + count, 0:width] = high
        ref[at : at + count, width : 2 * width] = (value - high.astype(F32)).astype(BF16)

    for d in range(dims):
        put(series_weights, d * LANES, jnp.transpose(diagonal[d]))

    state = []
    for v in range(var_count):
        parts = []
        for h in range(halves):
            parts.append(dofs[v, h * SUB : (h + 1) * SUB, :])
            if m_block > modes:
                parts.append(jnp.zeros((SUB, m_block - modes), F32))
        state.append(jnp.concatenate(parts, axis=1))

    def mixed(coef, value):
        return [
            [
                total_of(
                    [coef[d, v * var_count + w] * value[w] for w in range(var_count)]
                )
                for v in range(var_count)
            ]
            for d in range(dims)
        ]

    def step(coef, value):
        return product(mixed(coef, value), series_weights[...])

    first_weights = taylor_weights(0.0, fine_step, ORDER)
    second_weights = taylor_weights(fine_step, 2.0 * fine_step, ORDER)

    for h in range(halves):
        for f in range(faces):
            at = h * LANES + f * j_block
            spread_projection[
                at : at + face_modes, h * m_block : h * m_block + modes
            ] = projection[:, f, :]
    put(face_weights, 0, jnp.transpose(spread_projection[...]))
    for d in range(dims):
        put(back_weights, d * LANES, diagonal[d])
    put(back_weights, dims * LANES, -spread_projection[...])
    whole = spread_projection[0:LANES, :]
    for h in range(1, halves):
        whole = whole + spread_projection[h * LANES : (h + 1) * LANES, :]
    put(both_weights, 0, -whole)

    for f in range(faces):
        at = slice(f * j_block, f * j_block + elems)
        ints[0:1, at] = face_source[f : f + 1, :]
        ints[1:2, at] = fault_faces[f : f + 1, :]
    ints[2:3, 0:elems] = levels[...]
    ints[3:4, 0:slots] = send_source[...]

    raw = row_of(ints, 0)
    beyond = jnp.maximum(raw - faces * elems, 0)
    code_delta = beyond // (n_sub * slots) - 1
    code_turn = lax.rem((beyond // slots) % n_sub - me_sub + n_sub, n_sub)
    code_slot = beyond % slots
    own_export = take(row_of(ints, 3), code_slot)
    is_far = raw >= faces * elems
    is_own = is_far & (code_delta == 0) & (code_turn == 0)
    local_code = jnp.where(is_own, own_export, jnp.where(is_far, -1, raw))
    far_code = jnp.where(
        is_far & jnp.logical_not(is_own),
        ((code_delta + 1) * n_sub + code_turn) * slots + code_slot,
        -1,
    )
    local_index, local_elem, far_index, far_place = [], [], [], []
    for h in range(halves):
        local = take(local_code, flux_index[h])
        far = take(far_code, flux_index[h])
        near_by = jnp.maximum(local, 0)
        there = jnp.maximum(far, 0)
        local_index.append((near_by // elems) * j_block + inside)
        local_elem.append(jnp.where(local < 0, -1, near_by % elems))
        far_index.append((there % slots) * j_block + inside)
        far_place.append(jnp.where(far < 0, -1, there // slots + n_sub))
    sent = take(row_of(ints, 3), block)
    sent_index = (sent // elems) * j_block + inside
    sent_elem = sent % elems
    small = take(row_of(ints, 3), lane_slot)
    small_elem = small % elems
    rising = take(row_of(ints, 3), sub_slot) % elems

    exported_code = take(local_code, block * j_block + rising)
    exported_index = (jnp.maximum(exported_code, 0) // elems) * j_block + inside
    exported_elem = jnp.where(
        exported_code < 0, -1, jnp.maximum(exported_code, 0) % elems
    )

    square[0:var_count, 0:var_count] = fault_flux[...]
    turned = jnp.transpose(square[...])[0 : up_to(var_count, SUB)]
    for v in range(var_count):
        column = jnp.broadcast_to(turned[:, v : v + 1], (turned.shape[0], LANES))
        fault_rows[v * var_count : (v + 1) * var_count, :] = column[0:var_count]
    def send(source, target, partners, index_of, send_sem, recv_sem):
        for delta, turn in partners:
            pltpu.make_async_remote_copy(
                src_ref=source,
                dst_ref=target(index_of(-delta, -turn % n_sub)),
                send_sem=send_sem.at[0],
                recv_sem=recv_sem.at[0],
                device_id=device(delta, turn),
                device_id_type=MESH,
            ).start()

    def settle(whole, sem):
        pltpu.make_async_copy(whole, whole, sem.at[0]).wait()

    def near_place(delta, turn):
        return near.index((delta, turn))

    early_at = 3
    current, firsts = state, [first_weights[0] * tile for tile in state]
    seconds = [second_weights[0] * tile for tile in state]
    for term in range(1, ORDER):
        if term == 2:
            loads[9].wait()
            lines(plus_lines, flux_plus, faces)
            on_fault = jnp.broadcast_to(ints[1:2, :], packed_plus.shape) == 1
            packed_plus[...] = jnp.where(on_fault, fault_rows[...], pack(plus_lines, faces))

            part_of = inside // slots
            early_star = jnp.minimum(part_of, dims - 1) * j_block + small_elem
            early_plus = jnp.clip(part_of - dims, 0, faces - 1) * j_block + small_elem
            for i in range(deep // SUB):
                value = jnp.zeros((SUB, LANES), F32)
                for q in range(quarters):
                    at = slice(q * deep + i * SUB, q * deep + (i + 1) * SUB)
                    one = jnp.where(
                        part_of < dims,
                        take(packed_star[at, :], early_star),
                        take(packed_plus[at, :], early_plus),
                    )
                    value = jnp.where(block == q, one, value)
                early_out[i * SUB : (i + 1) * SUB, :] = value
            marks = [
                take(far_code, block * j_block + small_elem),
                jnp.where(take(row_of(ints, 2), sent_elem) == 0, 1, 0),
                small // elems,
            ]
            for i, mark in enumerate(marks):
                early_out[deep + i : deep + i + 1, :] = mark[0:1].astype(F32)

        if term == early_at:
            pl.semaphore_wait(barrier, len(wide))
            send(
                early_out,
                lambda at: early_in.at[at],
                near,
                near_place,
                early_send,
                early_recv,
            )
            loads[10].wait()
            lines(minus_lines, flux_minus, faces)
            packed_minus[...] = pack(minus_lines, faces)
            for i, ref in enumerate((packed_minus, packed_plus)):
                for pair in range(pairs):
                    exported_coef[i, pair] = take(
                        row_of(ref, pair), block * j_block + rising
                    )
        current = step(star_coef, current)
        firsts = [a + first_weights[term] * b for a, b in zip(firsts, current)]
        seconds = [a + second_weights[term] * b for a, b in zip(seconds, current)]
    first_half, second_half = firsts, seconds

    def face_values(value):
        broad = product([value], face_weights[...])
        return [
            [tile[:, h * LANES : (h + 1) * LANES] for h in range(halves)]
            for tile in broad
        ]

    def export(ref, at, values):
        for v in range(var_count):
            picked = total_of(
                [
                    jnp.where(
                        sent_elem == h * SUB + sublane, take(values[v][h], sent_index), 0.0
                    )
                    for h in range(halves)
                ]
            )
            ref[at + v : at + v + 1, :] = jnp.sum(picked, axis=0, keepdims=True)

    def flux_of(coef, values):
        return [
            total_of([coef[v * var_count + w] * values[w] for w in range(var_count)])
            for v in range(var_count)
        ]

    def gather_shifted(rows, maps):
        result = []
        for shifts in maps:
            parts = []
            for turn, source in enumerate(shifts):
                one = jnp.where(source == 0, rows[0], 0.0)
                for at in range(1, len(rows)):
                    one = jnp.where(source == at, rows[at], one)
                parts.append(pltpu.roll(one, turn * j_block, 1) if turn else one)
            result.append(total_of(parts))
        return result

    def gather_local(ref, elem_map):
        beside = [[jnp.zeros((SUB, LANES), F32)] * var_count for _ in range(halves)]
        for h in range(halves):
            for v in range(var_count):
                for e in range(elems):
                    row = row_of(ref.at[v, e // SUB], e % SUB)
                    beside[h][v] = jnp.where(
                        elem_map[h] == e, take(row, local_index[h]), beside[h][v]
                    )
        return beside

    values = face_values(first_half)
    export(first_out, 0, values)
    send(
        first_out, lambda at: first_in.at[at], wide, place, first_send, first_recv
    )
    own_place = place(0, 0)
    first_in[own_place] = first_out[...]

    def pulled(ref, elem):
        result = []
        for v in range(var_count):
            row = jnp.zeros((SUB, LANES), F32)
            for e in range(SUB):
                row = jnp.where(elem % SUB == e, row_of(ref.at[v], e), row)
            one = row
            for turn in range(1, halves):
                moved_row = pltpu.roll(row, turn * m_block, 1)
                one = jnp.where((elem // SUB + turn) % halves == mode_half, moved_row, one)
            result.append(one)
        return result

    volume = product(mixed(star_coef, first_half), back_weights[0 : dims * LANES, :])
    for v in range(var_count):
        part_ref[0, v] = state[v] + volume[v]
        for h in range(halves):
            faces_ref[0, v, h] = values[v][h]
    exported_state = pulled(part_ref.at[0], rising)
    own, other = [], []
    for v in range(var_count):
        one = jnp.zeros((SUB, LANES), F32)
        two = one
        for e in range(elems):
            row = row_of(faces_ref.at[0, v, e // SUB], e % SUB)
            one = jnp.where(rising == e, row, one)
            two = jnp.where(exported_elem == e, take(row, exported_index), two)
        own.append(one)
        other.append(two)
    flux = [
        a + b
        for a, b in zip(
            flux_of(exported_coef.at[0], own), flux_of(exported_coef.at[1], other)
        )
    ]
    rising_state = [
        a + b for a, b in zip(exported_state, product([flux], both_weights[...]))
    ]
    nears = -(-var_count // per_set)
    for t in range(nears):
        value = jnp.zeros((SUB, LANES), F32)
        for part in range(per_set):
            v = t * per_set + part
            if v < var_count:
                here = (sub_stack == part % stack) & (mode_half == part // stack)
                value = jnp.where(here, rising_state[v], value)
        near_out[t * SUB : (t + 1) * SUB, :] = value
    last_parts = min(var_count - (nears - 1) * per_set, stack)
    near_rows = (nears - 1) * SUB + last_parts * slots
    send(
        near_out.at[0:near_rows],
        lambda at: near_in.at[at, 0:near_rows],
        near,
        near_place,
        near_send,
        near_recv,
    )
    second_values = face_values(second_half)
    export(second_out, 0, second_values)
    send(
        second_out,
        lambda at: second_in.at[at],
        near,
        near_place,
        second_send,
        second_recv,
    )
    is_fine = (row_of(ints, 2) == 0) & (lane < elems)
    below = lax.broadcasted_iota(jnp.int32, (LANES, LANES), 1)
    flags = jnp.where(is_fine, 1.0, 0.0)
    rank = dot(
        jnp.concatenate([flags, flags], axis=0).astype(BF16),
        jnp.where(from_lane < below, 1.0, 0.0).astype(BF16),
    )[0:SUB].astype(jnp.int32)
    fine_rank = jnp.where(is_fine, rank, -1)
    fine_elem = jnp.sum(
        jnp.where(fine_rank == sublane, lane.astype(F32), 0.0), axis=1, keepdims=True
    )
    fine_elem = jnp.broadcast_to(fine_elem, (SUB, LANES))
    fine_across = jnp.sum(jnp.where(keep, fine_elem, 0.0), axis=0, keepdims=True)
    fine_across = jnp.broadcast_to(fine_across, (SUB, LANES)).astype(jnp.int32)
    fine_elem = fine_elem.astype(jnp.int32)
    home = take(fine_rank, star_index)
    local_rank, coarse_elem = [], []
    for h in range(halves):
        source = take(fine_rank, jnp.maximum(local_elem[h], 0))
        local_rank.append(jnp.where(local_elem[h] < 0, -1, source))
        coarse_elem.append(jnp.where(local_rank[h] < 0, local_elem[h], -1))

    def shifted(index, elem):
        result = []
        for turn in range(quarters):
            away = (block - index // j_block + quarters) % quarters
            kept = jnp.where(away == turn, elem, -1)
            result.append(
                pltpu.roll(kept, (quarters - turn) % quarters * j_block, 1)
                if turn
                else kept
            )
        return result

    home_faces = [take(fine_rank, h * SUB + sublane) for h in range(halves)]
    rank_shift = [shifted(a, b) for a, b in zip(local_index, local_rank)]

    for pair in range(pairs):
        row = row_of(packed_minus, pair)
        for h in range(halves):
            minus_coef[h, pair] = take(row, flux_index[h])
    for pair in range(pairs):
        row = row_of(packed_plus, pair)
        for h in range(halves):
            plus_coef[h, pair] = take(row, flux_index[h])
    beside = gather_local(faces_ref.at[0], local_elem)
    flux = []
    for h in range(halves):
        own = flux_of(minus_coef.at[h], [values[w][h] for w in range(var_count)])
        other = flux_of(plus_coef.at[h], beside[h])
        flux.append([a + b for a, b in zip(own, other)])
    partial = [
        a + b + c
        for a, b, c in zip(
            state, volume, product(flux, back_weights[dims * LANES :, :])
        )
    ]

    for v in range(var_count):
        part_ref[1, v] = partial[v]
    own_state = pulled(part_ref.at[1], fine_elem)
    for v in range(var_count):
        for h in range(halves):
            faces_ref[1, v, h] = second_values[v][h]
    coarse_beside = gather_local(faces_ref.at[1], coarse_elem)

    settle(early_in, early_recv)
    groups = -(-followed // per_group)
    for group in range(groups):
        members = range(group * per_group, min(followed, (group + 1) * per_group))
        for q in range(quarters):
            star_from = q * j_block + jnp.minimum(block, dims - 1) * slots + lane_slot
            plus_from = q * j_block + (dims + jnp.minimum(block, faces - 1)) * slots + lane_slot
            for i in range(deep // SUB):
                at = slice(q * deep + i * SUB, q * deep + (i + 1) * SUB)
                one = jnp.zeros((SUB, LANES), F32)
                two = one
                if group == 0:
                    here = part_of < stack
                    own = jnp.minimum(block, dims - 1) * j_block + fine_across
                    one = jnp.where(here, take(packed_star[at, :], own), one)
                    own = jnp.minimum(block, faces - 1) * j_block + fine_across
                    two = jnp.where(here, take(packed_plus[at, :], own), two)
                for k in members:
                    if k < stack:
                        continue
                    got = early_in[k - stack, i * SUB : (i + 1) * SUB, :]
                    here = part_of == k % per_group
                    one = jnp.where(here, take(got, star_from), one)
                    two = jnp.where(here, take(got, plus_from), two)
                guest_star[group, at, :] = one
                guest_plus[group, at, :] = two
    for group in range(groups):
        members = [s for s in range(sets) if s * per_set // per_group == group]
        picks = jnp.concatenate(
            [picks_of(s * per_set % per_group // stack, dims) for s in members], axis=1
        )
        for v in range(var_count):
            at = v * var_count
            rows = [row_of(guest_star.at[group], at + w) for w in range(var_count)]
            for w, tiles_of in enumerate(spread(rows, keep, picks)):
                for i, tile in enumerate(tiles_of):
                    guest_star_coef[members[i // dims], i % dims, at + w] = tile
    guest_far, guest_index, guest_face = [], [], []
    for t in range(tiles):
        member = t * stack + sub_stack
        index = (member % per_group) * slots + sub_slot + block * j_block
        group = t * stack // per_group
        for pair in range(pairs):
            row = row_of(guest_plus.at[group], pair)
            guest_plus_coef[t, pair] = take(row, index)
        code = jnp.full((SUB, LANES), -1, jnp.int32)
        face = jnp.zeros((SUB, LANES), jnp.int32)
        spin = jnp.zeros((SUB, LANES), jnp.int32)
        if t == 0:
            code = take(far_code, block * j_block + fine_elem)
        for part in range(stack):
            k = (t - 1) * stack + part
            if 0 <= k < len(near):
                here = sub_stack == part
                got = take(row_of(early_in.at[k], deep), block * j_block + sub_slot)
                code = jnp.where(here, got.astype(jnp.int32), code)
                got = take(row_of(early_in.at[k], deep + 2), sub_slot)
                face = jnp.where(here, got.astype(jnp.int32), face)
                spin = jnp.where(here, near[k][1], spin)
        there = jnp.maximum(code, 0)
        step_delta = there // (n_sub * slots) - 1
        step_turn = lax.rem((there // slots) % n_sub + spin, n_sub)
        guest_index.append((there % slots) * j_block + inside)
        guest_far.append(jnp.where(code < 0, -1, (step_delta + 1) * n_sub + step_turn))
        guest_face.append(face * j_block + inside)

    def gather_far(sources, places, index, start):
        result = list(start)
        for v in range(var_count):
            for name, ref in sources:
                row = row_of(ref, v)
                result[v] = jnp.where(places == name, take(row, index), result[v])
        return result

    nothing = [jnp.zeros((SUB, LANES), F32)] * var_count
    settle(first_in.at[0 : len(wide)], first_recv)
    guest_change = []
    for s in range(sets):
        flux = []
        for h in range(halves):
            t = s * halves + h
            if t < tiles:
                base = near[(t - 1) * stack][0] if t else 0
                sources = [
                    ((d + 1) * n_sub + turn, first_in.at[place(base + d, turn)])
                    for d in (-1, 0, 1)
                    for turn in range(n_sub)
                ]
                got = gather_far(sources, guest_far[t], guest_index[t], nothing)
                flux.append(flux_of(guest_plus_coef.at[t], got))
        guest_change.append(
            product(flux, back_weights[dims * LANES : (dims + len(flux)) * LANES, :])
        )

    settle(near_in.at[:, 0:near_rows], near_recv)
    settle(second_in, second_recv)
    guest_state = []
    for s in range(sets):
        states = []
        for v in range(var_count):
            value = guest_change[s][v]
            t, part = v // per_set, v % per_set
            for h in range(halves):
                if s == 0 and h == 0:
                    value = jnp.where(mode_half == 0, value + own_state[v], value)
                    continue
                for j in range(stack):
                    k = s * per_set + (h - 1) * stack + j
                    if k < len(near):
                        got = near_in[k, t * SUB : (t + 1) * SUB, :]
                        if part % stack != j:
                            got = pltpu.roll(got, ((j - part % stack) * slots) % SUB, 0)
                        if part // stack != h:
                            got = pltpu.roll(
                                got, ((h - part // stack) * m_block) % LANES, 1
                            )
                        here = (sub_stack == j) & (mode_half == h)
                        value = jnp.where(here, value + got, value)
            states.append(value)
        guest_state.append(states)

    coefs = [guest_star_coef.at[s] for s in range(sets)]
    current = guest_state
    sums = [[first_weights[0] * tile for tile in value] for value in current]
    for term in range(1, ORDER):
        current = [step(coef, value) for coef, value in zip(coefs, current)]
        sums = [
            [a + first_weights[term] * b for a, b in zip(total, value)]
            for total, value in zip(sums, current)
        ]
    own_sources = [
        (place(delta, turn), first_in.at[place(delta, turn)])
        for delta in (-1, 0, 1)
        for turn in range(n_sub)
        if delta or turn
    ]
    first_far = [
        gather_far(own_sources, far_place[h], far_index[h], nothing)
        for h in range(halves)
    ]
    coarse_far, guest_at = [], []
    marks = [
        (place(delta, turn), early_in.at[k, deep + 1 : deep + 2])
        for k, (delta, turn) in enumerate(near)
    ]
    last_sources = [
        (place(delta, turn), second_in.at[k]) for k, (delta, turn) in enumerate(near)
    ]
    for h in range(halves):
        coarse_far.append(
            gather_far(last_sources, far_place[h], far_index[h], coarse_beside[h])
        )
        mark = jnp.zeros((SUB, LANES), F32)
        code = jnp.full((SUB, LANES), -1, jnp.int32)
        for k, (name, ref) in enumerate(marks):
            here = far_place[h] == name
            mark = jnp.where(here, take(row_of(ref, 0), far_index[h]), mark)
            code = jnp.where(here, k * slots + far_index[h] // j_block, code)
        guest_at.append(jnp.where(mark > 0.5, code, -1))

    guest_values = [face_values(total) for total in sums]
    for v in range(var_count):
        fine_ref[v] = guest_values[0][v][0]
    carried = []
    for v in range(var_count):
        one = sums[0][v]
        for h in range(1, halves):
            one = jnp.where(mode_half == h, pltpu.roll(sums[0][v], h * m_block, 1), one)
        part_ref[2, v] = one
        one = second_half[v]
        for rank_at in range(SUB):
            one = jnp.where(home == rank_at, row_of(part_ref.at[2, v], rank_at), one)
        carried.append(one)
    for s in range(sets):
        for h in range(halves):
            t = s * halves + h
            if 0 < t < tiles:
                for v in range(var_count):
                    guest_rows[t - 1, v] = take(guest_values[s][v][h], guest_face[t])
    fine_beside, values = [], []
    for v in range(var_count):
        rows = [row_of(fine_ref.at[v], at) for at in range(SUB)]
        ones = []
        for h in range(halves):
            one = second_values[v][h]
            for at in range(SUB):
                one = jnp.where(home_faces[h] == at, rows[at], one)
            ones.append(one)
        values.append(ones)
        if v < BY_TAKE:
            taken = []
            for h in range(halves):
                one = jnp.zeros((SUB, LANES), F32)
                for at in range(SUB):
                    got = take(rows[at], local_index[h])
                    one = jnp.where(local_rank[h] == at, got, one)
                taken.append(one)
            fine_beside.append(taken)
        else:
            fine_beside.append(gather_shifted(rows, rank_shift))
    volume = product(mixed(star_coef, carried), back_weights[0 : dims * LANES, :])
    flux = []
    for h in range(halves):
        got = []
        for v in range(var_count):
            one = coarse_far[h][v] + fine_beside[v][h]
            for at in range(len(near) * slots):
                row = row_of(guest_rows.at[at // SUB, v], at % SUB)
                one = jnp.where(guest_at[h] == at, row, one)
            got.append(one + first_far[h][v])
        own = flux_of(minus_coef.at[h], [values[w][h] for w in range(var_count)])
        other = flux_of(plus_coef.at[h], got)
        flux.append([a + b for a, b in zip(own, other)])
    result = [
        a + b + c
        for a, b, c in zip(
            partial, volume, product(flux, back_weights[dims * LANES :, :])
        )
    ]
    for v in range(var_count):
        for h in range(halves):
            out[v, h * SUB : (h + 1) * SUB, :] = result[v][
                :, h * m_block : h * m_block + modes
            ]
    settle(early_in, early_send)
    settle(first_in.at[0 : len(wide)], first_send)
    settle(second_in, second_send)
    settle(near_in.at[:, 0:near_rows], near_send)


def solution(mesh):
    n_dom, n_sub = mesh.shape["dom"], mesh.shape["sub"]

    def per_device(
        dofs,
        stiffness,
        projection,
        star,
        flux_minus,
        flux_plus,
        fault_flux,
        fault_faces,
        levels,
        face_source,
        send_source,
    ):
        var_count, modes, elems = dofs.shape
        dims = stiffness.shape[0]
        faces, face_modes = projection.shape[0], projection.shape[1]
        halves = elems // SUB
        pairs = var_count * var_count
        slots = send_source.shape[0]
        quarters = max(faces, slots)
        j_block = LANES // quarters
        deep = up_to(-(-pairs // quarters), SUB)
        count = quarters * deep
        pitch = max(dims, faces)
        near, wide = 3 * n_sub - 1, 5 * n_sub - 1
        stack = SUB // slots
        tiles = -(-(stack + near) // stack)
        sets = -(-tiles // halves)
        groups = -(-(stack + near) // (j_block // slots))
        near_rows = -(-var_count // (stack * halves)) * SUB
        moved = [
            jnp.transpose(dofs, (0, 2, 1)),
            stiffness,
            jnp.transpose(projection, (1, 0, 2)),
            jnp.transpose(star, (1, 2, 0, 3)),
            jnp.transpose(flux_minus, (1, 2, 0, 3)),
            jnp.transpose(flux_plus, (1, 2, 0, 3)),
            fault_flux,
            fault_faces,
            levels.reshape(1, -1),
            face_source,
            send_source.reshape(1, -1),
        ]
        result = pl.pallas_call(
            functools.partial(kernel, (n_dom, n_sub)),
            out_shape=pltpu.VMEM((var_count, elems, modes), F32),
            in_specs=[pl.BlockSpec(memory_space=pltpu.HBM)] * len(moved),
            out_specs=pl.BlockSpec(memory_space=pltpu.VMEM),
            scratch_shapes=[pltpu.VMEM(one.shape, one.dtype) for one in moved]
            + [
                pltpu.VMEM((count * pitch, LANES), F32),
                pltpu.VMEM((count * pitch, LANES), F32),
                pltpu.VMEM((count * pitch, LANES), F32),
                pltpu.VMEM((count, LANES), F32),
                pltpu.VMEM((count, LANES), F32),
                pltpu.VMEM((count, LANES), F32),
                pltpu.VMEM((SUB, LANES), jnp.int32),
                pltpu.VMEM((LANES, LANES), F32),
                pltpu.VMEM((count, LANES), F32),
                pltpu.VMEM((dims, LANES, LANES), F32),
                pltpu.VMEM((halves * LANES, LANES), F32),
                pltpu.VMEM((dims, pairs, SUB, LANES), F32),
                pltpu.VMEM((halves, pairs, SUB, LANES), F32),
                pltpu.VMEM((halves, pairs, SUB, LANES), F32),
                pltpu.VMEM((dims * LANES, 2 * LANES), BF16),
                pltpu.VMEM(((dims + halves) * LANES, 2 * LANES), BF16),
                pltpu.VMEM((LANES, 2 * halves * LANES), BF16),
                pltpu.VMEM((2, var_count, halves, SUB, LANES), F32),
                pltpu.VMEM((3, var_count, SUB, LANES), F32),
                pltpu.VMEM((var_count, SUB, LANES), F32),
                pltpu.VMEM((2, pairs, SUB, LANES), F32),
                pltpu.VMEM((LANES, 2 * LANES), BF16),
                pltpu.VMEM((groups, count, LANES), F32),
                pltpu.VMEM((groups, count, LANES), F32),
                pltpu.VMEM((sets, dims, pairs, SUB, LANES), F32),
                pltpu.VMEM((tiles, pairs, SUB, LANES), F32),
                pltpu.VMEM((tiles - 1, var_count, SUB, LANES), F32),
                pltpu.VMEM((deep + SUB, LANES), F32),
                pltpu.VMEM((near, deep + SUB, LANES), F32),
                pltpu.VMEM((near_rows, LANES), F32),
                pltpu.VMEM((near, near_rows, LANES), F32),
                pltpu.VMEM((var_count, LANES), F32),
                pltpu.VMEM((5 * n_sub, var_count, LANES), F32),
                pltpu.VMEM((var_count, LANES), F32),
                pltpu.VMEM((near, var_count, LANES), F32),
                pltpu.SemaphoreType.DMA((len(moved),)),
            ]
            + [pltpu.SemaphoreType.DMA((1,))] * 8,
            compiler_params=pltpu.CompilerParams(
                collective_id=0,
                has_side_effects=True,
                vmem_limit_bytes=66_000_000,
            ),
            name="window",
        )(*moved)
        return jnp.transpose(result, (0, 2, 1))

    return jax.shard_map(
        per_device,
        mesh=mesh,
        in_specs=(
            P(None, None, ("dom", "sub")),
            P(),
            P(),
            P(None, None, None, ("dom", "sub")),
            P(None, None, None, ("dom", "sub")),
            P(None, None, None, ("dom", "sub")),
            P(),
            P(None, ("dom", "sub")),
            P(("dom", "sub")),
            P(None, ("dom", "sub")),
            P(("dom", "sub")),
        ),
        out_specs=P(None, None, ("dom", "sub")),
        check_vma=False,
    )
```

```python
import functools
import math

import jax
import jax.numpy as jnp
from jax import lax
from jax.experimental import pallas as pl
from jax.experimental.pallas import tpu as pltpu
from jax.sharding import PartitionSpec as P

MESH = pl.DeviceIdType.MESH
ORDER = 6
fine_step = 0.75
F32 = jnp.float32
BF16 = jnp.bfloat16
SUB = 8
LANES = 128
BY_TAKE = 2


def taylor_weights(start_time, stop_time, term_count):
    return [
        (stop_time ** (term + 1) - start_time ** (term + 1)) / math.factorial(term + 1)
        for term in range(term_count)
    ]


def up_to(value, step):
    return -(-value // step) * step


def dot(a, b):
    return jnp.dot(a, b, preferred_element_type=F32)


def take(value, index):
    return jnp.take_along_axis(value, index, axis=1, mode="promise_in_bounds")


def total_of(parts):
    return functools.reduce(lambda a, b: a + b, parts)


def both(tiles):
    parts = []
    for tile in tiles:
        high = tile.astype(BF16).astype(F32)
        parts += [high, tile - high]
    return jnp.concatenate(parts, axis=0).astype(BF16)


def spread(rows, keep, picks):
    out = dot(both([jnp.where(keep, row, 0.0) for row in rows]), picks)
    blocks = picks.shape[1] // LANES
    return [
        [
            out[2 * SUB * i : 2 * SUB * i + SUB, b * LANES : (b + 1) * LANES]
            + out[2 * SUB * i + SUB : 2 * SUB * (i + 1), b * LANES : (b + 1) * LANES]
            for b in range(blocks)
        ]
        for i in range(len(rows))
    ]


def product(columns, weights):
    lhs = jnp.concatenate([both(tiles) for tiles in columns], axis=1)
    out = dot(lhs, weights)
    half = weights.shape[1] // 2
    result = []
    for v in range(len(columns[0])):
        at = 2 * SUB * v
        result.append(
            out[at : at + SUB, :half]
            + out[at : at + SUB, half:]
            + out[at + SUB : at + 2 * SUB, :half]
        )
    return result


def kernel(
    sizes,
    dofs_hbm,
    stiffness_hbm,
    projection_hbm,
    star_hbm,
    minus_hbm,
    plus_hbm,
    fault_hbm,
    fault_faces_hbm,
    levels_hbm,
    face_source_hbm,
    send_source_hbm,
    out,
    dofs,
    stiffness,
    projection,
    star,
    flux_minus,
    flux_plus,
    fault_flux,
    fault_faces,
    levels,
    face_source,
    send_source,
    star_lines,
    minus_lines,
    plus_lines,
    packed_star,
    packed_minus,
    packed_plus,
    ints,
    square,
    fault_rows,
    diagonal,
    spread_projection,
    star_coef,
    minus_coef,
    plus_coef,
    series_weights,
    back_weights,
    face_weights,
    faces_ref,
    part_ref,
    fine_ref,
    exported_coef,
    both_weights,
    guest_star,
    guest_plus,
    guest_star_coef,
    guest_plus_coef,
    guest_rows,
    early_out,
    early_in,
    near_out,
    near_in,
    first_out,
    first_in,
    second_out,
    second_in,
    load_sem,
    early_send,
    early_recv,
    near_send,
    near_recv,
    first_send,
    first_recv,
    second_send,
    second_recv,
):
    n_dom, n_sub = sizes
    var_count, elems, modes = dofs.shape
    dims = stiffness.shape[0]
    face_modes, faces = projection.shape[0], projection.shape[1]
    slots = send_source.shape[1]
    halves = elems // SUB
    m_block = LANES // halves
    j_block = LANES // max(faces, slots)
    quarters = LANES // j_block
    pairs = var_count * var_count
    pitch = star_lines.shape[0] // packed_star.shape[0]
    deep = packed_star.shape[0] // quarters
    stack = SUB // slots
    per_set = stack * halves
    per_group = j_block // slots

    near = [
        (delta, turn)
        for delta in (1, -1, 0)
        for turn in reversed(range(n_sub))
        if delta or turn
    ]
    wide = [
        (delta, turn)
        for delta in (1, 2, -1, -2, 0)
        for turn in reversed(range(n_sub))
        if delta or turn
    ]
    followed = stack + len(near)
    tiles = -(-followed // stack)
    sets = -(-tiles // halves)

    def place(delta, turn):
        return (delta + 2) * n_sub + turn % n_sub

    loads = [
        pltpu.make_async_copy(src, dst, load_sem.at[i])
        for i, (src, dst) in enumerate(
            (
                (star_hbm, star),
                (stiffness_hbm, stiffness),
                (dofs_hbm, dofs),
                (projection_hbm, projection),
                (face_source_hbm, face_source),
                (send_source_hbm, send_source),
                (levels_hbm, levels),
                (fault_faces_hbm, fault_faces),
                (fault_hbm, fault_flux),
                (plus_hbm, flux_plus),
                (minus_hbm, flux_minus),
            )
        )
    ]
    for load in loads:
        load.start()

    me_dom, me_sub = lax.axis_index("dom"), lax.axis_index("sub")

    def device(delta, turn):
        return (
            lax.rem(me_dom + delta + n_dom, n_dom),
            lax.rem(me_sub + turn, n_sub),
        )

    barrier = pltpu.get_barrier_semaphore()
    for delta, turn in wide:
        pl.semaphore_signal(
            barrier, inc=1, device_id=device(delta, turn), device_id_type=MESH
        )

    diagonal[...] = jnp.zeros_like(diagonal)
    spread_projection[...] = jnp.zeros_like(spread_projection)
    ints[...] = jnp.zeros_like(ints)
    square[...] = jnp.zeros_like(square)

    sublane = lax.broadcasted_iota(jnp.int32, (SUB, LANES), 0)
    lane = lax.broadcasted_iota(jnp.int32, (SUB, LANES), 1)
    mode_half = lane // m_block
    block = lane // j_block
    inside = lane % j_block
    lane_slot = lane % slots
    sub_slot = sublane % slots
    sub_stack = sublane // slots
    star_index = mode_half * SUB + sublane
    flux_index = [block * j_block + h * SUB + sublane for h in range(halves)]

    def row_of(ref, at):
        return jnp.broadcast_to(ref[at : at + 1, :], (SUB, LANES))

    loads[0].wait()

    def lines(ref, source, count):
        for v in range(var_count):
            for w in range(var_count):
                at = (v * var_count + w) * pitch
                ref[at : at + count, 0:elems] = source[v, w]

    def pack(ref, count):
        depth = packed_star.shape[0]
        where = lax.broadcasted_iota(jnp.int32, (depth, LANES), 1) // j_block
        value = ref[pl.ds(0, depth, stride=pitch), :]
        for f in range(1, count):
            part = ref[pl.ds(f, depth, stride=pitch), :]
            value = jnp.where(where == f, pltpu.roll(part, f * j_block, 1), value)
        return value

    for load in loads[1:9]:
        load.wait()
    lines(star_lines, star, dims)
    packed_star[...] = pack(star_lines, dims)
    from_lane = lax.broadcasted_iota(jnp.int32, (LANES, LANES), 0)
    to_half = lax.broadcasted_iota(jnp.int32, (LANES, LANES), 1) // m_block
    keep = lane % SUB == sublane

    def picks_of(first, count):
        return jnp.concatenate(
            [
                jnp.where(
                    (from_lane // j_block == d)
                    & (from_lane % j_block // SUB == first + to_half),
                    1.0,
                    0.0,
                )
                for d in range(count)
            ],
            axis=1,
        ).astype(BF16)

    by_matmul = min(dims, 2)
    own_picks = picks_of(0, by_matmul)
    for v in range(var_count):
        at = v * var_count
        rows = [row_of(packed_star, at + w) for w in range(var_count)]
        for w, tiles_of in enumerate(spread(rows, keep, own_picks)):
            for d, tile in enumerate(tiles_of):
                star_coef[d, at + w] = tile
    for d in range(by_matmul, dims):
        for pair in range(pairs):
            star_coef[d, pair] = take(row_of(star_lines, pair * pitch + d), star_index)

    for d in range(dims):
        for h in range(halves):
            at = slice(h * m_block, h * m_block + modes)
            diagonal[d, at, at] = stiffness[d]

    def put(ref, at, value):
        high = value.astype(BF16)
        count, width = value.shape
        ref[at : at + count, 0:width] = high
        ref[at : at + count, width : 2 * width] = (value - high.astype(F32)).astype(BF16)

    for d in range(dims):
        put(series_weights, d * LANES, jnp.transpose(diagonal[d]))

    state = []
    for v in range(var_count):
        parts = []
        for h in range(halves):
            parts.append(dofs[v, h * SUB : (h + 1) * SUB, :])
            if m_block > modes:
                parts.append(jnp.zeros((SUB, m_block - modes), F32))
        state.append(jnp.concatenate(parts, axis=1))

    def mixed(coef, value):
        return [
            [
                total_of(
                    [coef[d, v * var_count + w] * value[w] for w in range(var_count)]
                )
                for v in range(var_count)
            ]
            for d in range(dims)
        ]

    def step(coef, value):
        return product(mixed(coef, value), series_weights[...])

    first_weights = taylor_weights(0.0, fine_step, ORDER)
    second_weights = taylor_weights(fine_step, 2.0 * fine_step, ORDER)

    for h in range(halves):
        for f in range(faces):
            at = h * LANES + f * j_block
            spread_projection[
                at : at + face_modes, h * m_block : h * m_block + modes
            ] = projection[:, f, :]
    put(face_weights, 0, jnp.transpose(spread_projection[...]))
    for d in range(dims):
        put(back_weights, d * LANES, diagonal[d])
    put(back_weights, dims * LANES, -spread_projection[...])
    whole = spread_projection[0:LANES, :]
    for h in range(1, halves):
        whole = whole + spread_projection[h * LANES : (h + 1) * LANES, :]
    put(both_weights, 0, -whole)

    for f in range(faces):
        at = slice(f * j_block, f * j_block + elems)
        ints[0:1, at] = face_source[f : f + 1, :]
        ints[1:2, at] = fault_faces[f : f + 1, :]
    ints[2:3, 0:elems] = levels[...]
    ints[3:4, 0:slots] = send_source[...]

    raw = row_of(ints, 0)
    beyond = jnp.maximum(raw - faces * elems, 0)
    code_delta = beyond // (n_sub * slots) - 1
    code_turn = lax.rem((beyond // slots) % n_sub - me_sub + n_sub, n_sub)
    code_slot = beyond % slots
    own_export = take(row_of(ints, 3), code_slot)
    is_far = raw >= faces * elems
    is_own = is_far & (code_delta == 0) & (code_turn == 0)
    local_code = jnp.where(is_own, own_export, jnp.where(is_far, -1, raw))
    far_code = jnp.where(
        is_far & jnp.logical_not(is_own),
        ((code_delta + 1) * n_sub + code_turn) * slots + code_slot,
        -1,
    )
    local_index, local_elem, far_index, far_place = [], [], [], []
    for h in range(halves):
        local = take(local_code, flux_index[h])
        far = take(far_code, flux_index[h])
        near_by = jnp.maximum(local, 0)
        there = jnp.maximum(far, 0)
        local_index.append((near_by // elems) * j_block + inside)
        local_elem.append(jnp.where(local < 0, -1, near_by % elems))
        far_index.append((there % slots) * j_block + inside)
        far_place.append(jnp.where(far < 0, -1, there // slots + n_sub))
    sent = take(row_of(ints, 3), block)
    sent_index = (sent // elems) * j_block + inside
    sent_elem = sent % elems
    small = take(row_of(ints, 3), lane_slot)
    small_elem = small % elems
    rising = take(row_of(ints, 3), sub_slot) % elems

    exported_code = take(local_code, block * j_block + rising)
    exported_index = (jnp.maximum(exported_code, 0) // elems) * j_block + inside
    exported_elem = jnp.where(
        exported_code < 0, -1, jnp.maximum(exported_code, 0) % elems
    )

    square[0:var_count, 0:var_count] = fault_flux[...]
    turned = jnp.transpose(square[...])[0 : up_to(var_count, SUB)]
    for v in range(var_count):
        column = jnp.broadcast_to(turned[:, v : v + 1], (turned.shape[0], LANES))
        fault_rows[v * var_count : (v + 1) * var_count, :] = column[0:var_count]
    def send(source, target, partners, index_of, send_sem, recv_sem):
        for delta, turn in partners:
            pltpu.make_async_remote_copy(
                src_ref=source,
                dst_ref=target(index_of(-delta, -turn % n_sub)),
                send_sem=send_sem.at[0],
                recv_sem=recv_sem.at[0],
                device_id=device(delta, turn),
                device_id_type=MESH,
            ).start()

    def settle(whole, sem):
        pltpu.make_async_copy(whole, whole, sem.at[0]).wait()

    def near_place(delta, turn):
        return near.index((delta, turn))

    early_at = 3
    current, firsts = state, [first_weights[0] * tile for tile in state]
    seconds = [second_weights[0] * tile for tile in state]
    for term in range(1, ORDER):
        if term == 2:
            loads[9].wait()
            lines(plus_lines, flux_plus, faces)
            on_fault = jnp.broadcast_to(ints[1:2, :], packed_plus.shape) == 1
            packed_plus[...] = jnp.where(on_fault, fault_rows[...], pack(plus_lines, faces))

            part_of = inside // slots
            early_star = jnp.minimum(part_of, dims - 1) * j_block + small_elem
            early_plus = jnp.clip(part_of - dims, 0, faces - 1) * j_block + small_elem
            for i in range(deep // SUB):
                value = jnp.zeros((SUB, LANES), F32)
                for q in range(quarters):
                    at = slice(q * deep + i * SUB, q * deep + (i + 1) * SUB)
                    one = jnp.where(
                        part_of < dims,
                        take(packed_star[at, :], early_star),
                        take(packed_plus[at, :], early_plus),
                    )
                    value = jnp.where(block == q, one, value)
                early_out[i * SUB : (i + 1) * SUB, :] = value
            marks = [
                take(far_code, block * j_block + small_elem),
                jnp.where(take(row_of(ints, 2), sent_elem) == 0, 1, 0),
                small // elems,
            ]
            for i, mark in enumerate(marks):
                early_out[deep + i : deep + i + 1, :] = mark[0:1].astype(F32)

        if term == early_at:
            pl.semaphore_wait(barrier, len(wide))
            send(
                early_out,
                lambda at: early_in.at[at],
                near,
                near_place,
                early_send,
                early_recv,
            )
            loads[10].wait()
            lines(minus_lines, flux_minus, faces)
            packed_minus[...] = pack(minus_lines, faces)
            for i, ref in enumerate((packed_minus, packed_plus)):
                for pair in range(pairs):
                    exported_coef[i, pair] = take(
                        row_of(ref, pair), block * j_block + rising
                    )
        current = step(star_coef, current)
        firsts = [a + first_weights[term] * b for a, b in zip(firsts, current)]
        seconds = [a + second_weights[term] * b for a, b in zip(seconds, current)]
    first_half, second_half = firsts, seconds

    def face_values(value):
        broad = product([value], face_weights[...])
        return [
            [tile[:, h * LANES : (h + 1) * LANES] for h in range(halves)]
            for tile in broad
        ]

    def export(ref, at, values):
        for v in range(var_count):
            picked = total_of(
                [
                    jnp.where(
                        sent_elem == h * SUB + sublane, take(values[v][h], sent_index), 0.0
                    )
                    for h in range(halves)
                ]
            )
            ref[at + v : at + v + 1, :] = jnp.sum(picked, axis=0, keepdims=True)

    def flux_of(coef, values):
        return [
            total_of([coef[v * var_count + w] * values[w] for w in range(var_count)])
            for v in range(var_count)
        ]

    def gather_shifted(rows, maps):
        result = []
        for shifts in maps:
            parts = []
            for turn, source in enumerate(shifts):
                one = jnp.where(source == 0, rows[0], 0.0)
                for at in range(1, len(rows)):
                    one = jnp.where(source == at, rows[at], one)
                parts.append(pltpu.roll(one, turn * j_block, 1) if turn else one)
            result.append(total_of(parts))
        return result

    def gather_local(ref, elem_map):
        beside = [[jnp.zeros((SUB, LANES), F32)] * var_count for _ in range(halves)]
        for h in range(halves):
            for v in range(var_count):
                for e in range(elems):
                    row = row_of(ref.at[v, e // SUB], e % SUB)
                    beside[h][v] = jnp.where(
                        elem_map[h] == e, take(row, local_index[h]), beside[h][v]
                    )
        return beside

    values = face_values(first_half)
    export(first_out, 0, values)
    send(
        first_out, lambda at: first_in.at[at], wide, place, first_send, first_recv
    )
    own_place = place(0, 0)
    first_in[own_place] = first_out[...]

    def pulled(ref, elem):
        result = []
        for v in range(var_count):
            row = jnp.zeros((SUB, LANES), F32)
            for e in range(SUB):
                row = jnp.where(elem % SUB == e, row_of(ref.at[v], e), row)
            one = row
            for turn in range(1, halves):
                moved_row = pltpu.roll(row, turn * m_block, 1)
                one = jnp.where((elem // SUB + turn) % halves == mode_half, moved_row, one)
            result.append(one)
        return result

    volume = product(mixed(star_coef, first_half), back_weights[0 : dims * LANES, :])
    for v in range(var_count):
        part_ref[0, v] = state[v] + volume[v]
        for h in range(halves):
            faces_ref[0, v, h] = values[v][h]
    exported_state = pulled(part_ref.at[0], rising)
    own, other = [], []
    for v in range(var_count):
        one = jnp.zeros((SUB, LANES), F32)
        two = one
        for e in range(elems):
            row = row_of(faces_ref.at[0, v, e // SUB], e % SUB)
            one = jnp.where(rising == e, row, one)
            two = jnp.where(exported_elem == e, take(row, exported_index), two)
        own.append(one)
        other.append(two)
    flux = [
        a + b
        for a, b in zip(
            flux_of(exported_coef.at[0], own), flux_of(exported_coef.at[1], other)
        )
    ]
    rising_state = [
        a + b for a, b in zip(exported_state, product([flux], both_weights[...]))
    ]
    nears = -(-var_count // per_set)
    for t in range(nears):
        value = jnp.zeros((SUB, LANES), F32)
        for part in range(per_set):
            v = t * per_set + part
            if v < var_count:
                here = (sub_stack == part % stack) & (mode_half == part // stack)
                value = jnp.where(here, rising_state[v], value)
        near_out[t * SUB : (t + 1) * SUB, :] = value
    last_parts = min(var_count - (nears - 1) * per_set, stack)
    near_rows = (nears - 1) * SUB + last_parts * slots
    send(
        near_out.at[0:near_rows],
        lambda at: near_in.at[at, 0:near_rows],
        near,
        near_place,
        near_send,
        near_recv,
    )
    second_values = face_values(second_half)
    export(second_out, 0, second_values)
    send(
        second_out,
        lambda at: second_in.at[at],
        near,
        near_place,
        second_send,
        second_recv,
    )
    is_fine = (row_of(ints, 2) == 0) & (lane < elems)
    below = lax.broadcasted_iota(jnp.int32, (LANES, LANES), 1)
    flags = jnp.where(is_fine, 1.0, 0.0)
    rank = dot(
        jnp.concatenate([flags, flags], axis=0).astype(BF16),
        jnp.where(from_lane < below, 1.0, 0.0).astype(BF16),
    )[0:SUB].astype(jnp.int32)
    fine_rank = jnp.where(is_fine, rank, -1)
    fine_elem = jnp.sum(
        jnp.where(fine_rank == sublane, lane.astype(F32), 0.0), axis=1, keepdims=True
    )
    fine_elem = jnp.broadcast_to(fine_elem, (SUB, LANES))
    fine_across = jnp.sum(jnp.where(keep, fine_elem, 0.0), axis=0, keepdims=True)
    fine_across = jnp.broadcast_to(fine_across, (SUB, LANES)).astype(jnp.int32)
    fine_elem = fine_elem.astype(jnp.int32)
    home = take(fine_rank, star_index)
    local_rank, coarse_elem = [], []
    for h in range(halves):
        source = take(fine_rank, jnp.maximum(local_elem[h], 0))
        local_rank.append(jnp.where(local_elem[h] < 0, -1, source))
        coarse_elem.append(jnp.where(local_rank[h] < 0, local_elem[h], -1))

    def shifted(index, elem):
        result = []
        for turn in range(quarters):
            away = (block - index // j_block + quarters) % quarters
            kept = jnp.where(away == turn, elem, -1)
            result.append(
                pltpu.roll(kept, (quarters - turn) % quarters * j_block, 1)
                if turn
                else kept
            )
        return result

    home_faces = [take(fine_rank, h * SUB + sublane) for h in range(halves)]
    rank_shift = [shifted(a, b) for a, b in zip(local_index, local_rank)]

    for pair in range(pairs):
        row = row_of(packed_minus, pair)
        for h in range(halves):
            minus_coef[h, pair] = take(row, flux_index[h])
    for pair in range(pairs):
        row = row_of(packed_plus, pair)
        for h in range(halves):
            plus_coef[h, pair] = take(row, flux_index[h])
    beside = gather_local(faces_ref.at[0], local_elem)
    flux = []
    for h in range(halves):
        own = flux_of(minus_coef.at[h], [values[w][h] for w in range(var_count)])
        other = flux_of(plus_coef.at[h], beside[h])
        flux.append([a + b for a, b in zip(own, other)])
    partial = [
        a + b + c
        for a, b, c in zip(
            state, volume, product(flux, back_weights[dims * LANES :, :])
        )
    ]

    for v in range(var_count):
        part_ref[1, v] = partial[v]
    own_state = pulled(part_ref.at[1], fine_elem)
    for v in range(var_count):
        for h in range(halves):
            faces_ref[1, v, h] = second_values[v][h]
    coarse_beside = gather_local(faces_ref.at[1], coarse_elem)

    settle(early_in, early_recv)
    groups = -(-followed // per_group)
    for group in range(groups):
        members = range(group * per_group, min(followed, (group + 1) * per_group))
        for q in range(quarters):
            star_from = q * j_block + jnp.minimum(block, dims - 1) * slots + lane_slot
            plus_from = q * j_block + (dims + jnp.minimum(block, faces - 1)) * slots + lane_slot
            for i in range(deep // SUB):
                at = slice(q * deep + i * SUB, q * deep + (i + 1) * SUB)
                one = jnp.zeros((SUB, LANES), F32)
                two = one
                if group == 0:
                    here = part_of < stack
                    own = jnp.minimum(block, dims - 1) * j_block + fine_across
                    one = jnp.where(here, take(packed_star[at, :], own), one)
                    own = jnp.minimum(block, faces - 1) * j_block + fine_across
                    two = jnp.where(here, take(packed_plus[at, :], own), two)
                for k in members:
                    if k < stack:
                        continue
                    got = early_in[k - stack, i * SUB : (i + 1) * SUB, :]
                    here = part_of == k % per_group
                    one = jnp.where(here, take(got, star_from), one)
                    two = jnp.where(here, take(got, plus_from), two)
                guest_star[group, at, :] = one
                guest_plus[group, at, :] = two
    for group in range(groups):
        members = [s for s in range(sets) if s * per_set // per_group == group]
        picks = jnp.concatenate(
            [picks_of(s * per_set % per_group // stack, dims) for s in members], axis=1
        )
        for v in range(var_count):
            at = v * var_count
            rows = [row_of(guest_star.at[group], at + w) for w in range(var_count)]
            for w, tiles_of in enumerate(spread(rows, keep, picks)):
                for i, tile in enumerate(tiles_of):
                    guest_star_coef[members[i // dims], i % dims, at + w] = tile
    guest_far, guest_index, guest_face = [], [], []
    for t in range(tiles):
        member = t * stack + sub_stack
        index = (member % per_group) * slots + sub_slot + block * j_block
        group = t * stack // per_group
        for pair in range(pairs):
            row = row_of(guest_plus.at[group], pair)
            guest_plus_coef[t, pair] = take(row, index)
        code = jnp.full((SUB, LANES), -1, jnp.int32)
        face = jnp.zeros((SUB, LANES), jnp.int32)
        spin = jnp.zeros((SUB, LANES), jnp.int32)
        if t == 0:
            code = take(far_code, block * j_block + fine_elem)
        for part in range(stack):
            k = (t - 1) * stack + part
            if 0 <= k < len(near):
                here = sub_stack == part
                got = take(row_of(early_in.at[k], deep), block * j_block + sub_slot)
                code = jnp.where(here, got.astype(jnp.int32), code)
                got = take(row_of(early_in.at[k], deep + 2), sub_slot)
                face = jnp.where(here, got.astype(jnp.int32), face)
                spin = jnp.where(here, near[k][1], spin)
        there = jnp.maximum(code, 0)
        step_delta = there // (n_sub * slots) - 1
        step_turn = lax.rem((there // slots) % n_sub + spin, n_sub)
        guest_index.append((there % slots) * j_block + inside)
        guest_far.append(jnp.where(code < 0, -1, (step_delta + 1) * n_sub + step_turn))
        guest_face.append(face * j_block + inside)

    def gather_far(sources, places, index, start):
        result = list(start)
        for v in range(var_count):
            for name, ref in sources:
                row = row_of(ref, v)
                result[v] = jnp.where(places == name, take(row, index), result[v])
        return result

    nothing = [jnp.zeros((SUB, LANES), F32)] * var_count
    settle(first_in.at[0 : len(wide)], first_recv)
    guest_change = []
    for s in range(sets):
        flux = []
        for h in range(halves):
            t = s * halves + h
            if t < tiles:
                base = near[(t - 1) * stack][0] if t else 0
                sources = [
                    ((d + 1) * n_sub + turn, first_in.at[place(base + d, turn)])
                    for d in (-1, 0, 1)
                    for turn in range(n_sub)
                ]
                got = gather_far(sources, guest_far[t], guest_index[t], nothing)
                flux.append(flux_of(guest_plus_coef.at[t], got))
        guest_change.append(
            product(flux, back_weights[dims * LANES : (dims + len(flux)) * LANES, :])
        )

    settle(near_in.at[:, 0:near_rows], near_recv)
    settle(second_in, second_recv)
    guest_state = []
    for s in range(sets):
        states = []
        for v in range(var_count):
            value = guest_change[s][v]
            t, part = v // per_set, v % per_set
            for h in range(halves):
                if s == 0 and h == 0:
                    value = jnp.where(mode_half == 0, value + own_state[v], value)
                    continue
                for j in range(stack):
                    k = s * per_set + (h - 1) * stack + j
                    if k < len(near):
                        got = near_in[k, t * SUB : (t + 1) * SUB, :]
                        if part % stack != j:
                            got = pltpu.roll(got, ((j - part % stack) * slots) % SUB, 0)
                        if part // stack != h:
                            got = pltpu.roll(
                                got, ((h - part // stack) * m_block) % LANES, 1
                            )
                        here = (sub_stack == j) & (mode_half == h)
                        value = jnp.where(here, value + got, value)
            states.append(value)
        guest_state.append(states)

    coefs = [guest_star_coef.at[s] for s in range(sets)]
    current = guest_state
    sums = [[first_weights[0] * tile for tile in value] for value in current]
    for term in range(1, ORDER):
        current = [step(coef, value) for coef, value in zip(coefs, current)]
        sums = [
            [a + first_weights[term] * b for a, b in zip(total, value)]
            for total, value in zip(sums, current)
        ]
    own_sources = [
        (place(delta, turn), first_in.at[place(delta, turn)])
        for delta in (-1, 0, 1)
        for turn in range(n_sub)
        if delta or turn
    ]
    first_far = [
        gather_far(own_sources, far_place[h], far_index[h], nothing)
        for h in range(halves)
    ]
    coarse_far, guest_at = [], []
    marks = [
        (place(delta, turn), early_in.at[k, deep + 1 : deep + 2])
        for k, (delta, turn) in enumerate(near)
    ]
    last_sources = [
        (place(delta, turn), second_in.at[k]) for k, (delta, turn) in enumerate(near)
    ]
    for h in range(halves):
        coarse_far.append(
            gather_far(last_sources, far_place[h], far_index[h], coarse_beside[h])
        )
        mark = jnp.zeros((SUB, LANES), F32)
        code = jnp.full((SUB, LANES), -1, jnp.int32)
        for k, (name, ref) in enumerate(marks):
            here = far_place[h] == name
            mark = jnp.where(here, take(row_of(ref, 0), far_index[h]), mark)
            code = jnp.where(here, k * slots + far_index[h] // j_block, code)
        guest_at.append(jnp.where(mark > 0.5, code, -1))

    guest_values = [face_values(total) for total in sums]
    for v in range(var_count):
        fine_ref[v] = guest_values[0][v][0]
    carried = []
    for v in range(var_count):
        one = sums[0][v]
        for h in range(1, halves):
            one = jnp.where(mode_half == h, pltpu.roll(sums[0][v], h * m_block, 1), one)
        part_ref[2, v] = one
        one = second_half[v]
        for rank_at in range(SUB):
            one = jnp.where(home == rank_at, row_of(part_ref.at[2, v], rank_at), one)
        carried.append(one)
    for s in range(sets):
        for h in range(halves):
            t = s * halves + h
            if 0 < t < tiles:
                for v in range(var_count):
                    guest_rows[t - 1, v] = take(guest_values[s][v][h], guest_face[t])
    fine_beside, values = [], []
    for v in range(var_count):
        rows = [row_of(fine_ref.at[v], at) for at in range(SUB)]
        ones = []
        for h in range(halves):
            one = second_values[v][h]
            for at in range(SUB):
                one = jnp.where(home_faces[h] == at, rows[at], one)
            ones.append(one)
        values.append(ones)
        if v < BY_TAKE:
            taken = []
            for h in range(halves):
                one = jnp.zeros((SUB, LANES), F32)
                for at in range(SUB):
                    got = take(rows[at], local_index[h])
                    one = jnp.where(local_rank[h] == at, got, one)
                taken.append(one)
            fine_beside.append(taken)
        else:
            fine_beside.append(gather_shifted(rows, rank_shift))
    volume = product(mixed(star_coef, carried), back_weights[0 : dims * LANES, :])
    flux = []
    for h in range(halves):
        got = []
        for v in range(var_count):
            one = coarse_far[h][v] + fine_beside[v][h]
            for at in range(len(near) * slots):
                row = row_of(guest_rows.at[at // SUB, v], at % SUB)
                one = jnp.where(guest_at[h] == at, row, one)
            got.append(one + first_far[h][v])
        own = flux_of(minus_coef.at[h], [values[w][h] for w in range(var_count)])
        other = flux_of(plus_coef.at[h], got)
        flux.append([a + b for a, b in zip(own, other)])
    result = [
        a + b + c
        for a, b, c in zip(
            partial, volume, product(flux, back_weights[dims * LANES :, :])
        )
    ]
    for v in range(var_count):
        for h in range(halves):
            out[v, h * SUB : (h + 1) * SUB, :] = result[v][
                :, h * m_block : h * m_block + modes
            ]
    settle(early_in, early_send)
    settle(first_in.at[0 : len(wide)], first_send)
    settle(second_in, second_send)
    settle(near_in.at[:, 0:near_rows], near_send)


def solution(mesh):
    n_dom, n_sub = mesh.shape["dom"], mesh.shape["sub"]

    def per_device(
        dofs,
        stiffness,
        projection,
        star,
        flux_minus,
        flux_plus,
        fault_flux,
        fault_faces,
        levels,
        face_source,
        send_source,
    ):
        var_count, modes, elems = dofs.shape
        dims = stiffness.shape[0]
        faces, face_modes = projection.shape[0], projection.shape[1]
        halves = elems // SUB
        pairs = var_count * var_count
        slots = send_source.shape[0]
        quarters = max(faces, slots)
        j_block = LANES // quarters
        deep = up_to(-(-pairs // quarters), SUB)
        count = quarters * deep
        pitch = max(dims, faces)
        near, wide = 3 * n_sub - 1, 5 * n_sub - 1
        stack = SUB // slots
        tiles = -(-(stack + near) // stack)
        sets = -(-tiles // halves)
        groups = -(-(stack + near) // (j_block // slots))
        near_rows = -(-var_count // (stack * halves)) * SUB
        moved = [
            jnp.transpose(dofs, (0, 2, 1)),
            stiffness,
            jnp.transpose(projection, (1, 0, 2)),
            jnp.transpose(star, (1, 2, 0, 3)),
            jnp.transpose(flux_minus, (1, 2, 0, 3)),
            jnp.transpose(flux_plus, (1, 2, 0, 3)),
            fault_flux,
            fault_faces,
            levels.reshape(1, -1),
            face_source,
            send_source.reshape(1, -1),
        ]
        result = pl.pallas_call(
            functools.partial(kernel, (n_dom, n_sub)),
            out_shape=pltpu.VMEM((var_count, elems, modes), F32),
            in_specs=[pl.BlockSpec(memory_space=pltpu.HBM)] * len(moved),
            out_specs=pl.BlockSpec(memory_space=pltpu.VMEM),
            scratch_shapes=[pltpu.VMEM(one.shape, one.dtype) for one in moved]
            + [
                pltpu.VMEM((count * pitch, LANES), F32),
                pltpu.VMEM((count * pitch, LANES), F32),
                pltpu.VMEM((count * pitch, LANES), F32),
                pltpu.VMEM((count, LANES), F32),
                pltpu.VMEM((count, LANES), F32),
                pltpu.VMEM((count, LANES), F32),
                pltpu.VMEM((SUB, LANES), jnp.int32),
                pltpu.VMEM((LANES, LANES), F32),
                pltpu.VMEM((count, LANES), F32),
                pltpu.VMEM((dims, LANES, LANES), F32),
                pltpu.VMEM((halves * LANES, LANES), F32),
                pltpu.VMEM((dims, pairs, SUB, LANES), F32),
                pltpu.VMEM((halves, pairs, SUB, LANES), F32),
                pltpu.VMEM((halves, pairs, SUB, LANES), F32),
                pltpu.VMEM((dims * LANES, 2 * LANES), BF16),
                pltpu.VMEM(((dims + halves) * LANES, 2 * LANES), BF16),
                pltpu.VMEM((LANES, 2 * halves * LANES), BF16),
                pltpu.VMEM((2, var_count, halves, SUB, LANES), F32),
                pltpu.VMEM((3, var_count, SUB, LANES), F32),
                pltpu.VMEM((var_count, SUB, LANES), F32),
                pltpu.VMEM((2, pairs, SUB, LANES), F32),
                pltpu.VMEM((LANES, 2 * LANES), BF16),
                pltpu.VMEM((groups, count, LANES), F32),
                pltpu.VMEM((groups, count, LANES), F32),
                pltpu.VMEM((sets, dims, pairs, SUB, LANES), F32),
                pltpu.VMEM((tiles, pairs, SUB, LANES), F32),
                pltpu.VMEM((tiles - 1, var_count, SUB, LANES), F32),
                pltpu.VMEM((deep + SUB, LANES), F32),
                pltpu.VMEM((near, deep + SUB, LANES), F32),
                pltpu.VMEM((near_rows, LANES), F32),
                pltpu.VMEM((near, near_rows, LANES), F32),
                pltpu.VMEM((var_count, LANES), F32),
                pltpu.VMEM((5 * n_sub, var_count, LANES), F32),
                pltpu.VMEM((var_count, LANES), F32),
                pltpu.VMEM((near, var_count, LANES), F32),
                pltpu.SemaphoreType.DMA((len(moved),)),
            ]
            + [pltpu.SemaphoreType.DMA((1,))] * 8,
            compiler_params=pltpu.CompilerParams(
                collective_id=0,
                has_side_effects=True,
                vmem_limit_bytes=66_000_000,
            ),
            name="window",
        )(*moved)
        return jnp.transpose(result, (0, 2, 1))

    return jax.shard_map(
        per_device,
        mesh=mesh,
        in_specs=(
            P(None, None, ("dom", "sub")),
            P(),
            P(),
            P(None, None, None, ("dom", "sub")),
            P(None, None, None, ("dom", "sub")),
            P(None, None, None, ("dom", "sub")),
            P(),
            P(None, ("dom", "sub")),
            P(("dom", "sub")),
            P(None, ("dom", "sub")),
            P(("dom", "sub")),
        ),
        out_specs=P(None, None, ("dom", "sub")),
        check_vma=False,
    )
```
